128 devices in a mesh: tm: 8 (over z, core), lat: 16 (over x, y).
Axes of the slice: x: 4, y: 4, z: 4, core: 2. Of those that a mesh axis runs over, the one named last changes fastest.
Arguments:
- frames: bfloat16 [256, 512, 1024], P('tm', 'lat'), may hold values from -6 to 6
- projection: bfloat16 [256, 512, 256], P(('tm', 'lat')), may hold values from -0.25 to 0.25
- degree_range: int32 [256, 2], replicated, may hold values from 0 to 256, as said below
- offsets: int32 [8], replicated, may hold values from 0 to 63
Outputs:
- coupling: bfloat16 [256, 2, 8, 256, 2, 256], P(('tm', 'lat'))
The draws below stay inside these ranges and needn't reach their ends.
Inputs may be any that keep to these rules, and one draw needn't show every extreme that they name: `degree_range`: row m holds lo and hi with min(m, 255) <= lo < hi <= 256.
All inputs are finite; a program needn't handle non-finite values.
Results may differ from the reference program's by a relative error of at most 0.0093.
Values may be sent and summed in bfloat16 or wider, within the bound.
A program may use at most 64 MiB of HBM per device.

```python
import math
import jax
import jax.numpy as jnp
from jax import lax

FRAMES = 256
NLAT = 512
NLON = 1024
DEGREES = 256
ORDERS = 256
OFFSETS = 8


def draw_degree_range(key, part):
    lower_key = jax.random.fold_in(key, 11)
    upper_key = jax.random.fold_in(key, 23)
    orders = jnp.arange(ORDERS, dtype=jnp.int32)
    lower_bits = jax.random.randint(lower_key, (ORDERS,), 0, 1 << 20, dtype=jnp.int32)
    upper_bits = jax.random.randint(upper_key, (ORDERS,), 0, 1 << 20, dtype=jnp.int32)
    largest_width = max(DEGREES // 8, 1)
    lowest = jnp.minimum(orders + lower_bits % largest_width, DEGREES - 1)
    highest = lowest + 1 + upper_bits % (DEGREES - lowest)
    return jnp.stack([lowest, highest], axis=1).astype(jnp.int32)


def plant(entries, own_key, smallest, high):
    dims = entries.shape
    spot = [jax.random.randint(jax.random.fold_in(own_key, axis), (), 0, dims[axis]) for axis in range(len(dims))]
    entries = entries.at[tuple(spot)].set(smallest)
    longest = dims.index(max(dims))
    spot[longest] = (spot[longest] + 1) % dims[longest]
    return entries.at[tuple(spot)].set(high)


def steps_of(key, dims, cuts, low, high):
    level = 1.0
    for dim, parts in cuts:
        draws = jax.random.uniform(jax.random.fold_in(jax.random.fold_in(key, 6), dim), (parts,), jnp.float32, low / len(cuts), high / len(cuts))
        level = level * jnp.repeat(jnp.exp(draws), dims[dim] // parts).reshape((-1,) + (1,) * (len(dims) - 1 - dim))
    return level


def bell_draw(stream_key, dims, width, bound, shards=(), kind=jnp.bfloat16):
    values = jax.random.normal(stream_key, dims, jnp.float32) * width
    if len(shards) > 0:
        values = steps_of(stream_key, dims, shards, -0.22, 0.18) * values
    return jnp.clip(values, min=-bound, max=bound).astype(kind)


def setup_inputs(seed: int = 0) -> dict:
    keys = jax.random.split(jax.random.key(seed), 5)
    return {
        "frames": bell_draw(keys[0], (FRAMES, NLAT, NLON), 1.0, 6.0, ((0, 8), (1, 16))),
        "projection": bell_draw(keys[1], (ORDERS, NLAT, DEGREES), NLAT ** -0.5, 0.25, ((0, 128),)),
        "degree_range": draw_degree_range(jax.random.fold_in(keys[4], 71), 0),
        "offsets": plant(jax.random.randint(keys[3], (OFFSETS,), 0, FRAMES // 4), jax.random.fold_in(keys[3], 1), 0, (FRAMES // 4) - 1).astype(jnp.int32),
    }


def longitude_table(lon_count, order_ids):
    longitude_points = jnp.arange(lon_count, dtype=jnp.int32)
    rotation_radians = longitude_points[:, None] * order_ids[None, :] % lon_count
    angle = rotation_radians.astype(jnp.float32) * (2.0 * math.pi / lon_count)
    factor = 1.0 / math.sqrt(lon_count)
    table = jnp.stack([jnp.cos(angle) * factor, -jnp.sin(angle) * factor], axis=2)
    return table.reshape(lon_count, -1).astype(jnp.bfloat16)

def time_table(entry_total):
    observation_epochs = jnp.arange(entry_total, dtype=jnp.int32)
    rotation_radians = observation_epochs[:, None] * observation_epochs[None, :] % entry_total
    angle = rotation_radians.astype(jnp.float32) * (2.0 * math.pi / entry_total)
    factor = 1.0 / math.sqrt(entry_total)
    cosine = jnp.cos(angle) * factor
    sine = jnp.sin(angle) * factor
    upper = jnp.concatenate([cosine, sine], axis=1)
    lower = jnp.concatenate([-sine, cosine], axis=1)
    return jnp.concatenate([upper, lower], axis=0).astype(jnp.bfloat16)

def reference(frames, projection, degree_range, offsets):
    frame_count, colatitude_total, lon_count = frames.shape
    azimuthal_order_count, _, harmonic_degree_total = projection.shape
    table = longitude_table(lon_count, jnp.arange(azimuthal_order_count, dtype=jnp.int32))
    azimuthal = jnp.dot(frames.reshape(-1, lon_count), table, preferred_element_type=jnp.float32)
    azimuthal = azimuthal.astype(jnp.bfloat16).reshape(frame_count, colatitude_total, azimuthal_order_count, 2)
    by_order = jnp.transpose(azimuthal, (2, 0, 1, 3))
    degrees = jnp.arange(harmonic_degree_total, dtype=jnp.int32)
    keep = ((degrees[None, :] >= degree_range[:, 0:1]) & (degrees[None, :] < degree_range[:, 1:2])).astype(jnp.float32)
    transform = time_table(frame_count)

    def per_order(inputs):
        proj_one, spec_one, keep_one = inputs
        summed = jnp.einsum('tzp,zl->ptl', spec_one.astype(jnp.float32), proj_one.astype(jnp.float32))
        harmonic = (summed * keep_one[None, None, :]).astype(jnp.bfloat16).reshape(2 * frame_count, harmonic_degree_total)
        return jnp.dot(transform, harmonic, preferred_element_type=jnp.float32).astype(jnp.bfloat16)
    spectra = lax.map(per_order, (projection, by_order, keep))
    padded = jnp.concatenate([spectra, jnp.zeros((2, 2 * frame_count, harmonic_degree_total), jnp.bfloat16)], axis=0)
    factor = 1.0 / math.sqrt(frame_count)

    def mode_couple_share(order):
        own = lax.dynamic_index_in_dim(padded, order, 0, keepdims=False).astype(jnp.float32)
        partners = lax.dynamic_slice_in_dim(padded, order + 1, 2, 0).astype(jnp.float32)
        split = partners.reshape(2, 2, frame_count, harmonic_degree_total)
        doubled = jnp.concatenate([split, split], axis=2)
        results = []
        for displacement_position in range(offsets.shape[0]):
            start = (offsets[displacement_position] % frame_count).astype(jnp.int32)
            rolled = lax.dynamic_slice_in_dim(doubled, start, frame_count, 2)
            real_part = rolled.reshape(2, 2 * frame_count, harmonic_degree_total)
            imag_part = jnp.concatenate([rolled[:, 1], -rolled[:, 0]], axis=1)
            both = jnp.concatenate([real_part, imag_part], axis=2)
            results.append(jnp.einsum('rl,srm->slm', own, both))
        stacked = jnp.stack(results, axis=1) * factor
        return stacked.reshape(2, offsets.shape[0], harmonic_degree_total, 2, harmonic_degree_total).astype(jnp.bfloat16)
    return lax.map(mode_couple_share, jnp.arange(azimuthal_order_count, dtype=jnp.int32))
```

```python
import math

import jax
import jax.numpy as jnp
import numpy as np
from jax import lax
from jax.experimental import pallas as pl
from jax.experimental.pallas import tpu as pltpu
from jax.sharding import PartitionSpec as P

BF = jnp.bfloat16
F32 = jnp.float32


def longitude_table(lon_count, orders):
    pairs = orders // 2
    gh, op, gl = np.meshgrid(
        np.arange(pairs // 32), np.arange(4), np.arange(32), indexing="ij"
    )
    order = (2 * (32 * gh + gl) + op // 2).reshape(-1)
    part = (op % 2).reshape(-1)
    phase = np.arange(lon_count)[:, None] * order[None, :] % lon_count
    angle = phase * (2.0 * math.pi / lon_count)
    table = np.where(part[None, :] == 0, np.cos(angle), -np.sin(angle))
    return jnp.asarray((table / math.sqrt(lon_count)).astype(np.float32)).astype(BF)


def swap_index_and_lanes(values, unit):
    values = list(values)
    lane = lax.broadcasted_iota(jnp.int32, values[0].shape, 1)
    step = len(values) // 2
    while step:
        low = (lane & (step * unit)) == 0
        for i in range(len(values)):
            if i & step == 0:
                a, b = values[i], values[i + step]
                values[i] = jnp.where(low, a, pltpu.roll(b, step * unit, 1))
                values[i + step] = jnp.where(
                    low, pltpu.roll(a, 128 - step * unit, 1), b
                )
        step //= 2
    return values


def longitude_kernel(x_ref, table_ref, s_ref):
    for bh in range(2):
        rows = slice(16 * bh, 16 * bh + 16)
        lhs = x_ref[:, rows, :].reshape(512, 1024)
        for gp in range(2):
            z = jnp.dot(
                lhs, table_ref[:, 256 * gp : 256 * gp + 256], preferred_element_type=F32
            )
            z = z.astype(BF).reshape(32, 16, 256)
            for c in range(2):
                v = [z[t, :, 128 * c : 128 * c + 128] for t in range(32)]
                v = swap_index_and_lanes(v, 1)
                for gl in range(32):
                    s_ref[32 * (2 * gp + c) + gl, rows, :] = v[gl]


def latitude_kernel(range_ref, r_ref, proj_ref, h_ref, a_ref):
    @pl.loop(0, 32)
    def _(i):
        rows = pl.ds(pl.multiple_of(i * 16, 16), 16)
        for q in range(2):
            v = [r_ref[4 * q + j, rows, :] for j in range(4)]
            v = swap_index_and_lanes(v, 32)
            for op in range(4):
                lanes = slice(256 * (op % 2) + 128 * q, 256 * (op % 2) + 128 * q + 128)
                a_ref[op // 2, rows, lanes] = v[op]

    device = lax.axis_index("tm") * lax.axis_size("lat") + lax.axis_index("lat")
    degree = lax.broadcasted_iota(jnp.int32, (256, 512), 0)
    for o in range(2):
        h = lax.dot_general(
            proj_ref[o], a_ref[o], (((0,), (0,)), ((), ())), preferred_element_type=F32
        )
        low, high = range_ref[2 * device + o, 0], range_ref[2 * device + o, 1]
        keep = (degree >= low) & (degree < high)
        h_ref[o] = jnp.where(keep, h, 0.0).astype(BF)


def coupling_kernel(own_ref, next_ref, cos_ref, sin_ref, out_ref, twice_ref, partner_ref):
    o, k = pl.program_id(0), pl.program_id(1)

    @pl.when((o == 0) & (k == 0))
    def _():
        partner_ref[0] = own_ref[1]
        partner_ref[1] = next_ref[0]
        partner_ref[2] = next_ref[1]

    @pl.when(k == 0)
    def _():
        row = lax.broadcasted_iota(jnp.int32, (512, 256), 0)
        column = lax.broadcasted_iota(jnp.int32, (512, 256), 1)
        double = ((row >> 1) == column).astype(F32).astype(BF)
        twice_ref[...] = jnp.dot(double, own_ref[o], preferred_element_type=F32)

    cos = jnp.broadcast_to(cos_ref[k][None], (64, 8, 256)).reshape(512, 256)
    sin = jnp.broadcast_to(sin_ref[k][None], (64, 8, 256)).reshape(512, 256)
    real, imag = twice_ref[:, :256], twice_ref[:, 256:]
    left = jnp.concatenate(
        [
            (real * cos - imag * sin).astype(BF),
            (real * sin + imag * cos).astype(BF),
        ],
        axis=1,
    )
    for s in range(2):
        product = lax.dot_general(
            left,
            partner_ref[o + s],
            (((1,), (1,)), ((), ())),
            preferred_element_type=F32,
        )
        out_ref[0, s, 0] = product.astype(BF).reshape(256, 2, 256)


def whole(shape):
    return pl.BlockSpec(shape, lambda *_: (0,) * len(shape))


def phase_tables(offsets, frame_count):
    t = jnp.arange(frame_count, dtype=jnp.int32)
    turn = (offsets[:, None] * t[None, :]) % frame_count
    angle = turn.astype(F32) * (2.0 * math.pi / frame_count)
    scale = 1.0 / math.sqrt(frame_count)
    cos, sin = jnp.cos(angle) * scale, jnp.sin(angle) * scale
    odd = (jnp.arange(8) % 2 == 1)[None, :, None]
    return (
        jnp.where(odd, -sin[:, None], cos[:, None]),
        jnp.where(odd, cos[:, None], sin[:, None]),
    )


def shards(frames, projection, degree_range, offsets):
    table = longitude_table(1024, 256)
    sent = pl.pallas_call(
        longitude_kernel,
        out_shape=jax.ShapeDtypeStruct((128, 32, 128), BF),
        cost_estimate=pl.CostEstimate(
            flops=2**30, bytes_accessed=4 << 20, transcendentals=0
        ),
        name="longitude",
    )(frames, table)
    got = lax.all_to_all(sent, ("tm", "lat"), split_axis=0, concat_axis=0, tiled=True)
    harmonic = pl.pallas_call(
        latitude_kernel,
        in_specs=[
            pl.BlockSpec(memory_space=pltpu.SMEM),
            pl.BlockSpec(memory_space=pltpu.VMEM),
            pl.BlockSpec(memory_space=pltpu.VMEM),
        ],
        out_shape=jax.ShapeDtypeStruct((2, 256, 512), BF),
        scratch_shapes=[pltpu.VMEM((2, 512, 512), BF)],
        cost_estimate=pl.CostEstimate(
            flops=2**28, bytes_accessed=2 << 20, transcendentals=0
        ),
        name="latitude",
    )(degree_range, got.reshape(8, 512, 128), projection)
    devices = range(128)
    following = lax.ppermute(
        harmonic, ("tm", "lat"), [(i, i - 1) for i in devices if i > 0]
    )
    cos, sin = phase_tables(offsets, 256)
    return pl.pallas_call(
        coupling_kernel,
        grid=(2, 8),
        in_specs=[
            whole((2, 256, 512)),
            whole((2, 256, 512)),
            whole((8, 8, 256)),
            whole((8, 8, 256)),
        ],
        out_specs=pl.BlockSpec(
            (1, 2, 1, 256, 2, 256), lambda o, k: (o, 0, k, 0, 0, 0)
        ),
        out_shape=jax.ShapeDtypeStruct((2, 2, 8, 256, 2, 256), BF),
        scratch_shapes=[
            pltpu.VMEM((512, 512), F32),
            pltpu.VMEM((3, 256, 512), BF),
        ],
        cost_estimate=pl.CostEstimate(
            flops=2**32, bytes_accessed=10 << 20, transcendentals=0
        ),
        name="coupling",
    )(harmonic, following, cos, sin)


def solution(mesh):
    return jax.shard_map(
        shards,
        mesh=mesh,
        in_specs=(P("tm", "lat", None), P(("tm", "lat"), None, None), P(), P()),
        out_specs=P(("tm", "lat"), None, None, None, None, None),
        check_vma=False,
    )
```

```python
import math

import jax
import jax.numpy as jnp
import numpy as np
from jax import lax
from jax.experimental import pallas as pl
from jax.experimental.pallas import tpu as pltpu
from jax.sharding import PartitionSpec as P

BF = jnp.bfloat16
F32 = jnp.float32


def destination(chunk, slot):
    x, y, core = slot // 8, slot // 2 % 4, slot % 2
    z = (chunk + 8 - x - y) % 4
    return 2 * z + core, 4 * x + y


def longitude_table(lon_count):
    chunk, op, slot = np.meshgrid(
        np.arange(4), np.arange(4), np.arange(32), indexing="ij"
    )
    tm, lat = destination(chunk, slot)
    order = (2 * (16 * tm + lat) + op // 2).reshape(-1)
    part = (op % 2).reshape(-1)
    phase = np.arange(lon_count)[:, None] * order[None, :] % lon_count
    angle = phase * (2.0 * math.pi / lon_count)
    table = np.where(part[None, :] == 0, np.cos(angle), -np.sin(angle))
    return jnp.asarray((table / math.sqrt(lon_count)).astype(np.float32)).astype(BF)


def swap_index_and_lanes(values, unit):
    values = list(values)
    lane = lax.broadcasted_iota(jnp.int32, values[0].shape, 1)
    step = len(values) // 2
    while step:
        low = (lane & (step * unit)) == 0
        for i in range(len(values)):
            if i & step == 0:
                a, b = values[i], values[i + step]
                values[i] = jnp.where(low, a, pltpu.roll(b, step * unit, 1))
                values[i + step] = jnp.where(
                    low, pltpu.roll(a, 128 - step * unit, 1), b
                )
        step //= 2
    return values


def transform_kernel(
    range_ref, x_ref, table_ref, proj_ref, h_ref, s_ref, r_ref, a_ref, send_sem, recv_sem
):
    tm, lat = lax.axis_index("tm"), lax.axis_index("lat")
    me = 16 * tm + lat
    barrier = pltpu.get_barrier_semaphore()

    @pl.loop(1, 128)
    def _(i):
        peer = (me + i) % 128
        pl.semaphore_signal(barrier, inc=1, device_id=(peer // 16, peer % 16))

    for gp in range(2):
        for bh in range(2):
            rows = slice(16 * bh, 16 * bh + 16)
            z = jnp.dot(
                x_ref[:, rows, :].reshape(512, 1024),
                table_ref[:, 256 * gp : 256 * gp + 256],
                preferred_element_type=F32,
            )
            z = z.astype(BF).reshape(32, 16, 256)
            for c in range(2):
                v = [z[t, :, 128 * c : 128 * c + 128] for t in range(32)]
                v = swap_index_and_lanes(v, 1)
                for slot in range(32):
                    s_ref[32 * (2 * gp + c) + slot, rows, :] = v[slot]
        if gp == 0:
            pl.semaphore_wait(barrier, 127)

        @pl.loop(0, 64)
        def _(i):
            chunk, slot = 2 * gp + i % 2, (i // 2 + 2 * lat + tm) % 32
            to_tm, to_lat = destination(chunk, slot)

            @pl.when((to_tm != tm) | (to_lat != lat))
            def _():
                pltpu.make_async_remote_copy(
                    src_ref=s_ref.at[32 * chunk + slot],
                    dst_ref=r_ref.at[me],
                    send_sem=send_sem,
                    recv_sem=recv_sem,
                    device_id=(to_tm, to_lat),
                ).start()

    x, y = lat // 4, lat % 4
    mine = 32 * ((x + y + tm // 2) % 4) + 8 * x + 2 * y + tm % 2
    r_ref[me] = s_ref[mine]
    rest = pltpu.make_async_remote_copy(
        src_ref=s_ref.at[pl.ds(0, 127)],
        dst_ref=r_ref.at[pl.ds(0, 127)],
        send_sem=send_sem,
        recv_sem=recv_sem,
        device_id=(tm, lat),
    )
    rest.wait_recv()

    for i in range(32):
        rows = slice(16 * i, 16 * i + 16)
        for q in range(2):
            v = [
                r_ref[16 * (4 * q + j) + i // 2, 16 * (i % 2) : 16 * (i % 2) + 16, :]
                for j in range(4)
            ]
            v = swap_index_and_lanes(v, 32)
            for op in range(4):
                start = 256 * (op % 2) + 128 * q
                a_ref[op // 2, rows, start : start + 128] = v[op]
    degree = lax.broadcasted_iota(jnp.int32, (256, 512), 0)
    for o in range(2):
        h = lax.dot_general(
            proj_ref[o], a_ref[o], (((0,), (0,)), ((), ())), preferred_element_type=F32
        )
        low, high = range_ref[2 * me + o, 0], range_ref[2 * me + o, 1]
        keep = (degree >= low) & (degree < high)
        h_ref[o] = jnp.where(keep, h, 0.0).astype(BF)
    rest.wait_send()


def coupling_kernel(own_ref, next_ref, cos_ref, sin_ref, out_ref, twice_ref, partner_ref):
    o, k = pl.program_id(0), pl.program_id(1)

    @pl.when((o == 0) & (k == 0))
    def _():
        partner_ref[0] = own_ref[1]
        partner_ref[1] = next_ref[0]
        partner_ref[2] = next_ref[1]

    @pl.when(k == 0)
    def _():
        row = lax.broadcasted_iota(jnp.int32, (512, 256), 0)
        column = lax.broadcasted_iota(jnp.int32, (512, 256), 1)
        double = ((row >> 1) == column).astype(F32).astype(BF)
        twice_ref[...] = jnp.dot(double, own_ref[o], preferred_element_type=F32)

    cos = jnp.broadcast_to(cos_ref[k][None], (64, 8, 256)).reshape(512, 256)
    sin = jnp.broadcast_to(sin_ref[k][None], (64, 8, 256)).reshape(512, 256)
    real, imag = twice_ref[:, :256], twice_ref[:, 256:]
    left = jnp.concatenate(
        [
            (real * cos - imag * sin).astype(BF),
            (real * sin + imag * cos).astype(BF),
        ],
        axis=1,
    )
    for s in range(2):
        product = lax.dot_general(
            left,
            partner_ref[o + s],
            (((1,), (1,)), ((), ())),
            preferred_element_type=F32,
        )
        out_ref[0, s, 0] = product.astype(BF).reshape(256, 2, 256)


def whole(shape):
    return pl.BlockSpec(shape, lambda *_: (0,) * len(shape))


def phase_tables(offsets, frame_count):
    t = jnp.arange(frame_count, dtype=jnp.int32)
    turn = (offsets[:, None] * t[None, :]) % frame_count
    angle = turn.astype(F32) * (2.0 * math.pi / frame_count)
    scale = 1.0 / math.sqrt(frame_count)
    cos, sin = jnp.cos(angle) * scale, jnp.sin(angle) * scale
    odd = (jnp.arange(8) % 2 == 1)[None, :, None]
    return (
        jnp.where(odd, -sin[:, None], cos[:, None]),
        jnp.where(odd, cos[:, None], sin[:, None]),
    )


def shards(frames, projection, degree_range, offsets):
    harmonic = pl.pallas_call(
        transform_kernel,
        in_specs=[pl.BlockSpec(memory_space=pltpu.SMEM)]
        + [pl.BlockSpec(memory_space=pltpu.VMEM)] * 3,
        out_shape=jax.ShapeDtypeStruct((2, 256, 512), BF),
        scratch_shapes=[
            pltpu.VMEM((128, 32, 128), BF),
            pltpu.VMEM((128, 32, 128), BF),
            pltpu.VMEM((2, 512, 512), BF),
            pltpu.SemaphoreType.DMA,
            pltpu.SemaphoreType.DMA,
        ],
        compiler_params=pltpu.CompilerParams(collective_id=0, has_side_effects=True),
        cost_estimate=pl.CostEstimate(
            flops=2**30, bytes_accessed=4 << 20, transcendentals=0
        ),
        name="transform",
    )(degree_range, frames, longitude_table(1024), projection)
    devices = range(128)
    following = lax.ppermute(
        harmonic, ("tm", "lat"), [(i, i - 1) for i in devices if i > 0]
    )
    cos, sin = phase_tables(offsets, 256)
    return pl.pallas_call(
        coupling_kernel,
        grid=(2, 8),
        in_specs=[
            whole((2, 256, 512)),
            whole((2, 256, 512)),
            whole((8, 8, 256)),
            whole((8, 8, 256)),
        ],
        out_specs=pl.BlockSpec(
            (1, 2, 1, 256, 2, 256), lambda o, k: (o, 0, k, 0, 0, 0)
        ),
        out_shape=jax.ShapeDtypeStruct((2, 2, 8, 256, 2, 256), BF),
        scratch_shapes=[
            pltpu.VMEM((512, 512), F32),
            pltpu.VMEM((3, 256, 512), BF),
        ],
        cost_estimate=pl.CostEstimate(
            flops=2**32, bytes_accessed=10 << 20, transcendentals=0
        ),
        name="coupling",
    )(harmonic, following, cos, sin)


def solution(mesh):
    return jax.shard_map(
        shards,
        mesh=mesh,
        in_specs=(P("tm", "lat", None), P(("tm", "lat"), None, None), P(), P()),
        out_specs=P(("tm", "lat"), None, None, None, None, None),
        check_vma=False,
    )
```

```python
import math

import jax
import jax.numpy as jnp
import numpy as np
from jax import lax
from jax.experimental import pallas as pl
from jax.experimental.pallas import tpu as pltpu
from jax.sharding import PartitionSpec as P

BF = jnp.bfloat16
F32 = jnp.float32


def destination(chunk, slot):
    lat, core = slot >> 1, slot & 1
    return 2 * (chunk ^ (lat >> 2) ^ (lat & 3)) + core, lat


def longitude_table():
    chunk, op, slot = np.meshgrid(
        np.arange(4), np.arange(4), np.arange(32), indexing="ij"
    )
    tm, lat = destination(chunk, slot)
    order = (2 * (16 * tm + lat) + op // 2).reshape(-1)
    part = (op % 2).reshape(-1)
    phase = np.arange(1024)[:, None] * order[None, :] % 1024
    angle = phase * (2.0 * math.pi / 1024)
    table = np.where(part[None, :] == 0, np.cos(angle), -np.sin(angle))
    return jnp.asarray((table / 32.0).astype(np.float32)).astype(BF)


def swap_index_and_lanes(values, unit):
    values = list(values)
    lane = lax.broadcasted_iota(jnp.int32, values[0].shape, 1)
    step = len(values) // 2
    while step:
        low = (lane & (step * unit)) == 0
        for i in range(len(values)):
            if i & step == 0:
                a, b = values[i], values[i + step]
                values[i] = jnp.where(low, a, pltpu.roll(b, step * unit, 1))
                values[i + step] = jnp.where(
                    low, pltpu.roll(a, 128 - step * unit, 1), b
                )
        step //= 2
    return values


def transform_kernel(
    range_ref,
    x_hbm,
    table_hbm,
    proj_hbm,
    h_ref,
    x_ref,
    table_ref,
    proj_ref,
    flip_ref,
    s_ref,
    r_ref,
    a_ref,
    x_sem,
    table_sem,
    proj_sem,
    send_sem,
    recv_sem,
    pass_send_sem,
    pass_recv_sem,
):
    tm, lat = lax.axis_index("tm"), lax.axis_index("lat")
    me = 16 * tm + lat

    x_copies, table_copies = [], []
    for j in range(8):
        lanes = pl.ds(128 * j, 128)
        x_copies.append(
            pltpu.make_async_copy(x_hbm.at[:, :, lanes], x_ref.at[j], x_sem.at[j])
        )
    for j in range(2):
        lanes = pl.ds(256 * j, 256)
        table_copies.append(
            pltpu.make_async_copy(
                table_hbm.at[:, lanes], table_ref.at[j], table_sem.at[j]
            )
        )
    proj_copy = pltpu.make_async_copy(proj_hbm, proj_ref, proj_sem)
    table_copies[0].start()
    for copy in x_copies:
        copy.start()
    table_copies[1].start()
    proj_copy.start()

    barrier = pltpu.get_barrier_semaphore()

    @pl.loop(1, 128, unroll=4)
    def _(i):
        pl.semaphore_signal(barrier, inc=1, device_id=(tm ^ (i >> 4), lat ^ (i & 15)))

    table_copies[0].wait()
    for copy in x_copies:
        copy.wait()
    for gp in range(2):
        if gp == 1:
            table_copies[1].wait()
        for bh in range(2):
            rows = slice(16 * bh, 16 * bh + 16)
            x = jnp.concatenate(
                [x_ref[j, :, rows, :].reshape(512, 128) for j in range(8)], axis=1
            )
            z = jnp.dot(x, table_ref[gp], preferred_element_type=F32)
            z = z.astype(BF).reshape(32, 16, 256)
            for c in range(2):
                v = [z[t, :, 128 * c : 128 * c + 128] for t in range(32)]
                v = swap_index_and_lanes(v, 1)
                for slot in range(32):
                    s_ref[32 * (2 * gp + c) + slot, rows, :] = v[slot]
        if gp == 0:
            pl.semaphore_wait(barrier, 127)

        @pl.loop(0, 64, unroll=4)
        def _(i):
            chunk, slot = 2 * gp + (i & 1), (i >> 1) ^ (2 * lat + (tm & 1))
            to_tm, to_lat = destination(chunk, slot)

            @pl.when((to_tm != tm) | (to_lat != lat))
            def _():
                pltpu.make_async_remote_copy(
                    src_ref=s_ref.at[32 * chunk + slot],
                    dst_ref=r_ref.at[me],
                    send_sem=send_sem,
                    recv_sem=recv_sem,
                    device_id=(to_tm, to_lat),
                ).start()

    mine = 32 * ((tm >> 1) ^ (lat >> 2) ^ (lat & 3)) + 2 * lat + (tm & 1)
    r_ref[me] = s_ref[mine]
    proj_copy.wait()
    for o in range(2):
        flip_ref[o] = proj_ref[o].T
    rest = pltpu.make_async_remote_copy(
        src_ref=s_ref.at[pl.ds(0, 127)],
        dst_ref=r_ref.at[pl.ds(0, 127)],
        send_sem=send_sem,
        recv_sem=recv_sem,
        device_id=(tm, lat),
    )
    rest.wait_recv()

    for i in range(32):
        rows = slice(16 * i, 16 * i + 16)
        for q in range(2):
            v = [
                r_ref[16 * (4 * q + j) + i // 2, 16 * (i % 2) : 16 * (i % 2) + 16, :]
                for j in range(4)
            ]
            v = swap_index_and_lanes(v, 32)
            for op in range(4):
                a_ref[op // 2, 2 * (op % 2) + q, rows, :] = v[op]
    degree = lax.broadcasted_iota(jnp.int32, (256, 512), 0)
    before = jnp.maximum(me - 1, 0)
    passes = []
    for o in range(2):
        columns = jnp.concatenate([a_ref[o, j] for j in range(4)], axis=1)
        h = jnp.dot(flip_ref[o], columns, preferred_element_type=F32)
        low, high = range_ref[0, 2 * me + o], range_ref[1, 2 * me + o]
        keep = (degree >= low) & (degree < high)
        h_ref[o] = jnp.where(keep, h, 0.0).astype(BF)
        copy = pltpu.make_async_remote_copy(
            src_ref=h_ref.at[o],
            dst_ref=h_ref.at[2 + o],
            send_sem=pass_send_sem.at[o],
            recv_sem=pass_recv_sem.at[o],
            device_id=(before >> 4, before & 15),
        )
        passes.append(copy)

        @pl.when(me > 0)
        def _():
            copy.start()

    rest.wait_send()

    @pl.when(me == 127)
    def _():
        h_ref[2] = jnp.zeros((256, 512), BF)
        h_ref[3] = jnp.zeros((256, 512), BF)

    @pl.when(me < 127)
    def _():
        for copy in passes:
            copy.wait_recv()

    @pl.when(me > 0)
    def _():
        for copy in passes:
            copy.wait_send()


def phases(offset):
    row = lax.broadcasted_iota(jnp.int32, (8, 256), 0)
    t = lax.broadcasted_iota(jnp.int32, (8, 256), 1)
    turn = (offset * t + 64 * (row & 1)) & 255
    angle = turn.astype(F32) * (2.0 * math.pi / 256)
    return jnp.cos(angle) * (1.0 / 16), jnp.sin(angle) * (1.0 / 16)


def coupling_kernel(
    offsets_ref, h_ref, out_ref, twice_ref, cos_ref, sin_ref, left_ref
):
    o, pair = pl.program_id(0), pl.program_id(1)

    def build(slot, k):
        cos = jnp.broadcast_to(cos_ref[k][None], (64, 8, 256)).reshape(512, 256)
        sin = jnp.broadcast_to(sin_ref[k][None], (64, 8, 256)).reshape(512, 256)
        real, imag = twice_ref[:, :256], twice_ref[:, 256:]
        left_ref[slot, :, :256] = (real * cos - imag * sin).astype(BF)
        left_ref[slot, :, 256:] = (real * sin + imag * cos).astype(BF)

    def multiply(slot):
        for s in range(2):
            product = lax.dot_general(
                left_ref[slot],
                h_ref[o + 1 + s],
                (((1,), (1,)), ((), ())),
                preferred_element_type=F32,
            )
            out_ref[0, s, slot] = product.astype(BF).reshape(256, 2, 256)

    @pl.when((o == 0) & (pair == 0))
    def _():
        for k in range(8):
            cos, sin = phases(offsets_ref[k])
            cos_ref[k] = cos
            sin_ref[k] = sin

    @pl.when(pair == 0)
    def _():
        row = lax.broadcasted_iota(jnp.int32, (512, 256), 0)
        column = lax.broadcasted_iota(jnp.int32, (512, 256), 1)
        double = ((row >> 1) == column).astype(F32).astype(BF)
        twice_ref[...] = jnp.dot(double, h_ref[o], preferred_element_type=F32)
        build(0, 0)

    build(1, 2 * pair + 1)
    multiply(0)
    build(0, jnp.minimum(2 * pair + 2, 7))
    multiply(1)


def shards(frames, projection, degree_range, offsets):
    anywhere = pl.BlockSpec(memory_space=pl.ANY)
    spectra = pl.pallas_call(
        transform_kernel,
        in_specs=[pl.BlockSpec(memory_space=pltpu.SMEM)] + [anywhere] * 3,
        out_specs=pl.BlockSpec(memory_space=pltpu.VMEM),
        out_shape=jax.ShapeDtypeStruct((4, 256, 512), BF),
        scratch_shapes=[
            pltpu.VMEM((8, 32, 32, 128), BF),
            pltpu.VMEM((2, 1024, 256), BF),
            pltpu.VMEM((2, 512, 256), BF),
            pltpu.VMEM((2, 256, 512), BF),
            pltpu.VMEM((128, 32, 128), BF),
            pltpu.VMEM((128, 32, 128), BF),
            pltpu.VMEM((2, 4, 512, 128), BF),
            pltpu.SemaphoreType.DMA((8,)),
            pltpu.SemaphoreType.DMA((2,)),
            pltpu.SemaphoreType.DMA,
            pltpu.SemaphoreType.DMA,
            pltpu.SemaphoreType.DMA,
            pltpu.SemaphoreType.DMA((2,)),
            pltpu.SemaphoreType.DMA((2,)),
        ],
        compiler_params=pltpu.CompilerParams(collective_id=0, has_side_effects=True),
        cost_estimate=pl.CostEstimate(
            flops=2**30, bytes_accessed=4 << 20, transcendentals=0
        ),
        name="transform",
    )(degree_range.T, frames, longitude_table(), projection)
    return pl.pallas_call(
        coupling_kernel,
        grid=(2, 4),
        in_specs=[
            pl.BlockSpec(memory_space=pltpu.SMEM),
            pl.BlockSpec((4, 256, 512), lambda o, pair: (0, 0, 0)),
        ],
        out_specs=pl.BlockSpec(
            (1, 2, 2, 256, 2, 256), lambda o, pair: (o, 0, pair, 0, 0, 0)
        ),
        out_shape=jax.ShapeDtypeStruct((2, 2, 8, 256, 2, 256), BF),
        scratch_shapes=[
            pltpu.VMEM((512, 512), F32),
            pltpu.VMEM((8, 8, 256), F32),
            pltpu.VMEM((8, 8, 256), F32),
            pltpu.VMEM((2, 512, 512), BF),
        ],
        cost_estimate=pl.CostEstimate(
            flops=2**32, bytes_accessed=10 << 20, transcendentals=0
        ),
        name="coupling",
    )(offsets, spectra)


def solution(mesh):
    return jax.shard_map(
        shards,
        mesh=mesh,
        in_specs=(P("tm", "lat", None), P(("tm", "lat"), None, None), P(), P()),
        out_specs=P(("tm", "lat"), None, None, None, None, None),
        check_vma=False,
    )
```

```python
import math

import jax
import jax.numpy as jnp
import numpy as np
from jax import lax
from jax.experimental import pallas as pl
from jax.experimental.pallas import tpu as pltpu
from jax.sharding import PartitionSpec as P

BF = jnp.bfloat16
F32 = jnp.float32


def longitude_table():
    group, op, slot = np.meshgrid(
        np.arange(4), np.arange(4), np.arange(32), indexing="ij"
    )
    order = (2 * (32 * group + slot) + op // 2).reshape(-1)
    part = (op % 2).reshape(-1)
    phase = np.arange(1024)[:, None] * order[None, :] % 1024
    angle = phase * (2.0 * math.pi / 1024)
    table = np.where(part[None, :] == 0, np.cos(angle), -np.sin(angle))
    return jnp.asarray((table / 32.0).astype(np.float32)).astype(BF)


def swap_index_and_lanes(values, unit):
    values = list(values)
    lane = lax.broadcasted_iota(jnp.int32, values[0].shape, 1)
    step = len(values) // 2
    while step:
        low = (lane & (step * unit)) == 0
        for i in range(len(values)):
            if i & step == 0:
                a, b = values[i], values[i + step]
                values[i] = jnp.where(low, a, pltpu.roll(b, step * unit, 1))
                values[i + step] = jnp.where(
                    low, pltpu.roll(a, 128 - step * unit, 1), b
                )
        step //= 2
    return values


def transform_kernel(
    range_ref,
    x_hbm,
    table_hbm,
    proj_hbm,
    h_ref,
    x_ref,
    table_ref,
    proj_ref,
    flip_ref,
    up_ref,
    across_ref,
    via_up_ref,
    via_across_ref,
    r_ref,
    a_ref,
    x_sem,
    table_sem,
    proj_sem,
    send_sem,
    recv_sem,
    pass_send_sem,
    pass_recv_sem,
):
    tm, lat = lax.axis_index("tm"), lax.axis_index("lat")
    me = 16 * tm + lat

    x_copies, table_copies = [], []
    for bh in range(2):
        for j in range(8):
            x_copies.append(
                pltpu.make_async_copy(
                    x_hbm.at[:, pl.ds(16 * bh, 16), pl.ds(128 * j, 128)],
                    x_ref.at[bh, j],
                    x_sem.at[bh, j],
                )
            )
    for j in range(2):
        table_copies.append(
            pltpu.make_async_copy(
                table_hbm.at[:, pl.ds(256 * j, 256)], table_ref.at[j], table_sem.at[j]
            )
        )
    proj_copy = pltpu.make_async_copy(proj_hbm, proj_ref, proj_sem)
    table_copies[0].start()
    for copy in x_copies[:8]:
        copy.start()
    table_copies[1].start()
    for copy in x_copies[8:]:
        copy.start()
    proj_copy.start()

    barrier = pltpu.get_barrier_semaphore()
    for i in range(1, 8):
        pl.semaphore_signal(barrier, inc=1, device_id=(tm ^ i, lat))
    for i in range(1, 16):
        pl.semaphore_signal(barrier, inc=1, device_id=(tm, lat ^ i))

    @pl.when((lat == 0) & (tm > 0))
    def _():
        pl.semaphore_signal(barrier, inc=1, device_id=(tm - 1, 15))

    @pl.when((lat == 15) & (tm < 7))
    def _():
        pl.semaphore_signal(barrier, inc=1, device_id=(tm + 1, 0))

    outside = ((lat == 0) & (tm > 0)) | ((lat == 15) & (tm < 7))

    def up(i, source, target, stage):
        return pltpu.make_async_remote_copy(
            src_ref=source,
            dst_ref=target,
            send_sem=send_sem.at[stage],
            recv_sem=recv_sem.at[stage],
            device_id=(tm ^ i, lat),
        )

    def across(i, source, target, stage):
        return pltpu.make_async_remote_copy(
            src_ref=source,
            dst_ref=target,
            send_sem=send_sem.at[stage],
            recv_sem=recv_sem.at[stage],
            device_id=(tm, lat ^ i),
        )

    for bh in range(2):
        for copy in x_copies[8 * bh : 8 * bh + 8]:
            copy.wait()
        for gp in range(2):
            if bh == 0:
                table_copies[gp].wait()
            x = jnp.concatenate(
                [x_ref[bh, j].reshape(512, 128) for j in range(8)], axis=1
            )
            z = jnp.dot(x, table_ref[gp], preferred_element_type=F32)
            z = z.astype(BF).reshape(32, 16, 256)
            for c in range(2):
                v = [z[t, :, 128 * c : 128 * c + 128] for t in range(32)]
                v = swap_index_and_lanes(v, 1)
                for slot in range(32):
                    to_tm, to_lat = 2 * (2 * gp + c) + slot // 16, slot % 16
                    if bh == 0:
                        up_ref[to_tm, to_lat] = v[slot]
                    else:
                        across_ref[to_lat, to_tm] = v[slot]
        if bh == 0:
            pl.semaphore_wait(barrier, 22 + outside.astype(jnp.int32))
            for i in range(1, 8):
                up(i, up_ref.at[tm ^ i], via_up_ref.at[tm], 0).start()
            via_up_ref[tm] = up_ref[tm]
        else:
            for i in range(1, 16):
                across(i, across_ref.at[lat ^ i], via_across_ref.at[lat], 1).start()
            via_across_ref[lat] = across_ref[lat]

    proj_copy.wait()
    for o in range(2):
        flip_ref[o] = proj_ref[o].T

    first = pl.ds(0, 7)
    up_all = up(0, up_ref.at[first], via_up_ref.at[first], 0)
    up_all.wait_recv()
    for i in range(1, 16):
        across(i, via_up_ref.at[:, lat ^ i], r_ref.at[:, lat, 0], 2).start()
    r_ref[:, lat, 0] = via_up_ref[:, lat]
    first = pl.ds(0, 15)
    across_all = across(0, across_ref.at[first], via_across_ref.at[first], 1)
    across_all.wait_recv()
    for i in range(1, 8):
        up(i, via_across_ref.at[:, tm ^ i], r_ref.at[tm, :, 1], 3).start()
    r_ref[tm, :, 1] = via_across_ref[:, tm]

    across_last = across(
        0, via_across_ref.at[pl.ds(0, 15)], r_ref.at[:, pl.ds(0, 15), 0], 2
    )
    up_last = up(0, via_up_ref.at[pl.ds(0, 7)], r_ref.at[pl.ds(0, 7), :, 1], 3)
    for half in range(2):
        if half == 0:
            across_last.wait_recv()
        else:
            up_last.wait_recv()
        for i in range(16):
            rows = slice(32 * i + 16 * half, 32 * i + 16 * half + 16)
            for q in range(2):
                v = [r_ref[4 * q + j, i, half] for j in range(4)]
                v = swap_index_and_lanes(v, 32)
                for op in range(4):
                    a_ref[op // 2, 2 * (op % 2) + q, rows, :] = v[op]
    degree = lax.broadcasted_iota(jnp.int32, (256, 512), 0)
    before = jnp.maximum(me - 1, 0)
    passes = []
    for o in range(2):
        columns = jnp.concatenate([a_ref[o, j] for j in range(4)], axis=1)
        h = jnp.dot(flip_ref[o], columns, preferred_element_type=F32)
        low, high = range_ref[0, 2 * me + o], range_ref[1, 2 * me + o]
        keep = (degree >= low) & (degree < high)
        h_ref[o] = jnp.where(keep, h, 0.0).astype(BF)
        copy = pltpu.make_async_remote_copy(
            src_ref=h_ref.at[o],
            dst_ref=h_ref.at[2 + o],
            send_sem=pass_send_sem.at[o],
            recv_sem=pass_recv_sem.at[o],
            device_id=(before >> 4, before & 15),
        )
        passes.append(copy)

        @pl.when(me > 0)
        def _():
            copy.start()

    up_all.wait_send()
    across_all.wait_send()
    across_last.wait_send()
    up_last.wait_send()

    @pl.when(me == 127)
    def _():
        h_ref[2] = jnp.zeros((256, 512), BF)
        h_ref[3] = jnp.zeros((256, 512), BF)

    @pl.when(me < 127)
    def _():
        for copy in passes:
            copy.wait_recv()

    @pl.when(me > 0)
    def _():
        for copy in passes:
            copy.wait_send()


def phases(offset):
    row = lax.broadcasted_iota(jnp.int32, (8, 256), 0)
    t = lax.broadcasted_iota(jnp.int32, (8, 256), 1)
    turn = (offset * t + 64 * (row & 1)) & 255
    angle = turn.astype(F32) * (2.0 * math.pi / 256)
    return jnp.cos(angle) * (1.0 / 16), jnp.sin(angle) * (1.0 / 16)


def coupling_kernel(
    offsets_ref, h_ref, out_ref, twice_ref, cos_ref, sin_ref, left_ref
):
    o, pair = pl.program_id(0), pl.program_id(1)

    def build(slot, k):
        cos = jnp.broadcast_to(cos_ref[k][None], (64, 8, 256)).reshape(512, 256)
        sin = jnp.broadcast_to(sin_ref[k][None], (64, 8, 256)).reshape(512, 256)
        real, imag = twice_ref[:, :256], twice_ref[:, 256:]
        left_ref[slot, :, :256] = (real * cos - imag * sin).astype(BF)
        left_ref[slot, :, 256:] = (real * sin + imag * cos).astype(BF)

    def multiply(slot):
        for s in range(2):
            product = lax.dot_general(
                left_ref[slot],
                h_ref[o + 1 + s],
                (((1,), (1,)), ((), ())),
                preferred_element_type=F32,
            )
            out_ref[0, s, slot] = product.astype(BF).reshape(256, 2, 256)

    @pl.when((o == 0) & (pair == 0))
    def _():
        for k in range(8):
            cos, sin = phases(offsets_ref[k])
            cos_ref[k] = cos
            sin_ref[k] = sin

    @pl.when(pair == 0)
    def _():
        row = lax.broadcasted_iota(jnp.int32, (512, 256), 0)
        column = lax.broadcasted_iota(jnp.int32, (512, 256), 1)
        double = ((row >> 1) == column).astype(F32).astype(BF)
        twice_ref[...] = jnp.dot(double, h_ref[o], preferred_element_type=F32)
        build(0, 0)

    build(1, 2 * pair + 1)
    multiply(0)
    build(0, jnp.minimum(2 * pair + 2, 7))
    multiply(1)


def shards(frames, projection, degree_range, offsets):
    anywhere = pl.BlockSpec(memory_space=pl.ANY)
    spectra = pl.pallas_call(
        transform_kernel,
        in_specs=[pl.BlockSpec(memory_space=pltpu.SMEM)] + [anywhere] * 3,
        out_specs=pl.BlockSpec(memory_space=pltpu.VMEM),
        out_shape=jax.ShapeDtypeStruct((4, 256, 512), BF),
        scratch_shapes=[
            pltpu.VMEM((2, 8, 32, 16, 128), BF),
            pltpu.VMEM((2, 1024, 256), BF),
            pltpu.VMEM((2, 512, 256), BF),
            pltpu.VMEM((2, 256, 512), BF),
            pltpu.VMEM((8, 16, 16, 128), BF),
            pltpu.VMEM((16, 8, 16, 128), BF),
            pltpu.VMEM((8, 16, 16, 128), BF),
            pltpu.VMEM((16, 8, 16, 128), BF),
            pltpu.VMEM((8, 16, 2, 16, 128), BF),
            pltpu.VMEM((2, 4, 512, 128), BF),
            pltpu.SemaphoreType.DMA((2, 8)),
            pltpu.SemaphoreType.DMA((2,)),
            pltpu.SemaphoreType.DMA,
            pltpu.SemaphoreType.DMA((4,)),
            pltpu.SemaphoreType.DMA((4,)),
            pltpu.SemaphoreType.DMA((2,)),
            pltpu.SemaphoreType.DMA((2,)),
        ],
        compiler_params=pltpu.CompilerParams(collective_id=0, has_side_effects=True),
        cost_estimate=pl.CostEstimate(
            flops=2**30, bytes_accessed=4 << 20, transcendentals=0
        ),
        name="transform",
    )(degree_range.T, frames, longitude_table(), projection)
    return pl.pallas_call(
        coupling_kernel,
        grid=(2, 4),
        in_specs=[
            pl.BlockSpec(memory_space=pltpu.SMEM),
            pl.BlockSpec((4, 256, 512), lambda o, pair: (0, 0, 0)),
        ],
        out_specs=pl.BlockSpec(
            (1, 2, 2, 256, 2, 256), lambda o, pair: (o, 0, pair, 0, 0, 0)
        ),
        out_shape=jax.ShapeDtypeStruct((2, 2, 8, 256, 2, 256), BF),
        scratch_shapes=[
            pltpu.VMEM((512, 512), F32),
            pltpu.VMEM((8, 8, 256), F32),
            pltpu.VMEM((8, 8, 256), F32),
            pltpu.VMEM((2, 512, 512), BF),
        ],
        cost_estimate=pl.CostEstimate(
            flops=2**32, bytes_accessed=10 << 20, transcendentals=0
        ),
        name="coupling",
    )(offsets, spectra)


def solution(mesh):
    return jax.shard_map(
        shards,
        mesh=mesh,
        in_specs=(P("tm", "lat", None), P(("tm", "lat"), None, None), P(), P()),
        out_specs=P(("tm", "lat"), None, None, None, None, None),
        check_vma=False,
    )
```

```python
import math

import jax
import jax.numpy as jnp
import numpy as np
from jax import lax
from jax.experimental import pallas as pl
from jax.experimental.pallas import tpu as pltpu
from jax.sharding import PartitionSpec as P

BF = jnp.bfloat16
F32 = jnp.float32


def longitude_table():
    group, op, slot = np.meshgrid(
        np.arange(4), np.arange(4), np.arange(32), indexing="ij"
    )
    order = (2 * (32 * group + slot) + op // 2).reshape(-1)
    part = (op % 2).reshape(-1)
    phase = np.arange(1024)[:, None] * order[None, :] % 1024
    angle = phase * (2.0 * math.pi / 1024)
    table = np.where(part[None, :] == 0, np.cos(angle), -np.sin(angle))
    return jnp.asarray((table / 32.0).astype(np.float32)).astype(BF)


def farthest_first(count, fields):
    def hops(i):
        return sum((0, 1, 2, 1)[i >> shift & 3] for shift in fields)

    return sorted(range(1, count), key=lambda i: (-hops(i), i))


UP = farthest_first(8, (1,))
ACROSS = farthest_first(16, (0, 2))


def swap_index_and_lanes(values, unit):
    values = list(values)
    lane = lax.broadcasted_iota(jnp.int32, values[0].shape, 1)
    step = len(values) // 2
    while step:
        low = (lane & (step * unit)) == 0
        for i in range(len(values)):
            if i & step == 0:
                a, b = values[i], values[i + step]
                values[i] = jnp.where(low, a, pltpu.roll(b, step * unit, 1))
                values[i + step] = jnp.where(
                    low, pltpu.roll(a, 128 - step * unit, 1), b
                )
        step //= 2
    return values


def transform_kernel(
    range_ref,
    offsets_ref,
    x_hbm,
    table_hbm,
    proj_hbm,
    h_ref,
    left_ref,
    x_ref,
    table_ref,
    proj_ref,
    flip_ref,
    up_ref,
    across_ref,
    via_up_ref,
    via_across_ref,
    r_ref,
    a_ref,
    twice_ref,
    x_sem,
    table_sem,
    proj_sem,
    send_sem,
    recv_sem,
    pass_send_sem,
    pass_recv_sem,
):
    tm, lat = lax.axis_index("tm"), lax.axis_index("lat")
    me = 16 * tm + lat

    x_copies, table_copies = [], []
    for bh in range(2):
        for j in range(8):
            x_copies.append(
                pltpu.make_async_copy(
                    x_hbm.at[:, pl.ds(16 * bh, 16), pl.ds(128 * j, 128)],
                    x_ref.at[bh, j],
                    x_sem.at[bh, j],
                )
            )
    for j in range(2):
        table_copies.append(
            pltpu.make_async_copy(
                table_hbm.at[:, pl.ds(256 * j, 256)], table_ref.at[j], table_sem.at[j]
            )
        )
    proj_copy = pltpu.make_async_copy(proj_hbm, proj_ref, proj_sem)
    table_copies[0].start()
    for copy in x_copies[:8]:
        copy.start()
    table_copies[1].start()
    for copy in x_copies[8:]:
        copy.start()
    proj_copy.start()

    barrier = pltpu.get_barrier_semaphore()
    for i in range(1, 8):
        pl.semaphore_signal(barrier, inc=1, device_id=(tm ^ i, lat))
    for i in range(1, 16):
        pl.semaphore_signal(barrier, inc=1, device_id=(tm, lat ^ i))

    @pl.when((lat == 0) & (tm > 0))
    def _():
        pl.semaphore_signal(barrier, inc=1, device_id=(tm - 1, 15))

    @pl.when((lat == 15) & (tm < 7))
    def _():
        pl.semaphore_signal(barrier, inc=1, device_id=(tm + 1, 0))

    outside = ((lat == 0) & (tm > 0)) | ((lat == 15) & (tm < 7))

    def up(i, source, target, stage):
        return pltpu.make_async_remote_copy(
            src_ref=source,
            dst_ref=target,
            send_sem=send_sem.at[stage],
            recv_sem=recv_sem.at[stage],
            device_id=(tm ^ i, lat),
        )

    def across(i, source, target, stage):
        return pltpu.make_async_remote_copy(
            src_ref=source,
            dst_ref=target,
            send_sem=send_sem.at[stage],
            recv_sem=recv_sem.at[stage],
            device_id=(tm, lat ^ i),
        )

    for bh in range(2):
        for copy in x_copies[8 * bh : 8 * bh + 8]:
            copy.wait()
        for gp in range(2):
            if bh == 0:
                table_copies[gp].wait()
            x = jnp.concatenate(
                [x_ref[bh, j].reshape(512, 128) for j in range(8)], axis=1
            )
            z = jnp.dot(x, table_ref[gp], preferred_element_type=F32)
            z = z.astype(BF).reshape(32, 16, 256)
            for c in range(2):
                v = [z[t, :, 128 * c : 128 * c + 128] for t in range(32)]
                v = swap_index_and_lanes(v, 1)
                for slot in range(32):
                    to_tm, to_lat = 2 * (2 * gp + c) + slot // 16, slot % 16
                    if bh == 0:
                        up_ref[to_tm, to_lat] = v[slot]
                    else:
                        across_ref[to_lat, to_tm] = v[slot]
    pl.semaphore_wait(barrier, 22 + outside.astype(jnp.int32))
    for i in ACROSS[:8]:
        across(i, across_ref.at[lat ^ i], via_across_ref.at[lat], 1).start()
    for i in UP:
        up(i, up_ref.at[tm ^ i], via_up_ref.at[tm], 0).start()
    for i in ACROSS[8:]:
        across(i, across_ref.at[lat ^ i], via_across_ref.at[lat], 1).start()
    via_up_ref[tm] = up_ref[tm]
    via_across_ref[lat] = across_ref[lat]

    proj_copy.wait()
    for o in range(2):
        flip_ref[o] = proj_ref[o].T

    some = pl.ds(0, 7)
    up_all = up(0, up_ref.at[some], via_up_ref.at[some], 0)
    up_all.wait_recv()
    for i in ACROSS:
        across(i, via_up_ref.at[:, lat ^ i], r_ref.at[:, lat, 0], 2).start()
    some = pl.ds(0, 15)
    across_all = across(0, across_ref.at[some], via_across_ref.at[some], 1)
    across_all.wait_recv()
    for i in UP:
        up(i, via_across_ref.at[:, tm ^ i], r_ref.at[tm, :, 1], 3).start()
    r_ref[:, lat, 0] = via_up_ref[:, lat]
    r_ref[tm, :, 1] = via_across_ref[:, tm]

    across_last = across(
        0, via_across_ref.at[pl.ds(0, 15)], r_ref.at[:, pl.ds(0, 15), 0], 2
    )
    up_last = up(0, via_up_ref.at[pl.ds(0, 7)], r_ref.at[pl.ds(0, 7), :, 1], 3)
    for half in range(2):
        if half == 0:
            across_last.wait_recv()
        else:
            up_last.wait_recv()
        for i in range(16):
            rows = slice(32 * i + 16 * half, 32 * i + 16 * half + 16)
            for q in range(2):
                v = [r_ref[4 * q + j, i, half] for j in range(4)]
                v = swap_index_and_lanes(v, 32)
                for op in range(4):
                    a_ref[op // 2, 2 * (op % 2) + q, rows, :] = v[op]
    degree = lax.broadcasted_iota(jnp.int32, (256, 512), 0)
    before = jnp.maximum(me - 1, 0)

    def passed(o, c):
        rows = pl.ds(32 * c, 32)
        return pltpu.make_async_remote_copy(
            src_ref=h_ref.at[o, rows],
            dst_ref=h_ref.at[2 + o, rows],
            send_sem=pass_send_sem.at[o, c],
            recv_sem=pass_recv_sem.at[o, c],
            device_id=(before >> 4, before & 15),
        )

    for o in range(2):
        columns = jnp.concatenate([a_ref[o, j] for j in range(4)], axis=1)
        h = jnp.dot(flip_ref[o], columns, preferred_element_type=F32)
        low, high = range_ref[0, 2 * me + o], range_ref[1, 2 * me + o]
        keep = (degree >= low) & (degree < high)
        h_ref[o] = jnp.where(keep, h, 0.0).astype(BF)
        for c in range(8):

            @pl.when((me > 0) & (32 * (c + 1) > 2 * me + o))
            def _():
                passed(o, c).start()

    up_all.wait_send()
    across_all.wait_send()
    across_last.wait_send()
    up_last.wait_send()

    row = lax.broadcasted_iota(jnp.int32, (512, 256), 0)
    column = lax.broadcasted_iota(jnp.int32, (512, 256), 1)
    double = ((row >> 1) == column).astype(F32).astype(BF)
    for o in range(2):
        twice_ref[o] = jnp.dot(double, h_ref[o], preferred_element_type=F32)

    @pl.loop(0, 8)
    def _(k):
        cos, sin = phases(offsets_ref[k])
        cos = jnp.broadcast_to(cos[None], (64, 8, 256)).reshape(512, 256)
        sin = jnp.broadcast_to(sin[None], (64, 8, 256)).reshape(512, 256)
        for o in range(2):
            real, imag = twice_ref[o, :, :256], twice_ref[o, :, 256:]
            left_ref[o, k, :, :256] = (real * cos - imag * sin).astype(BF)
            left_ref[o, k, :, 256:] = (real * sin + imag * cos).astype(BF)

    for o in range(2):
        for c in range(8):
            sent = (me < 127) & (32 * (c + 1) > 2 * (me + 1) + o)

            @pl.when(sent)
            def _():
                passed(o, c).wait_recv()

            @pl.when(jnp.logical_not(sent))
            def _():
                h_ref[2 + o, 32 * c : 32 * c + 32] = jnp.zeros((32, 512), BF)

            @pl.when((me > 0) & (32 * (c + 1) > 2 * me + o))
            def _():
                passed(o, c).wait_send()


def phases(offset):
    row = lax.broadcasted_iota(jnp.int32, (8, 256), 0)
    t = lax.broadcasted_iota(jnp.int32, (8, 256), 1)
    turn = (offset * t + 64 * (row & 1)) & 255
    angle = turn.astype(F32) * (2.0 * math.pi / 256)
    return jnp.cos(angle) * (1.0 / 16), jnp.sin(angle) * (1.0 / 16)


def coupling_kernel(left_ref, h_ref, out_ref):
    o = pl.program_id(0)
    for s in range(2):
        product = lax.dot_general(
            left_ref[0].reshape(1024, 512),
            h_ref[o + 1 + s],
            (((1,), (1,)), ((), ())),
            preferred_element_type=F32,
        )
        out_ref[0, s] = product.astype(BF).reshape(2, 256, 2, 256)


def shards(frames, projection, degree_range, offsets):
    anywhere = pl.BlockSpec(memory_space=pltpu.HBM)
    far = [
        pltpu.with_memory_space_constraint(a, pltpu.HBM)
        for a in (degree_range.T, offsets, frames, longitude_table(), projection)
    ]
    spectra, left = pl.pallas_call(
        transform_kernel,
        in_specs=[pl.BlockSpec(memory_space=pltpu.SMEM)] * 2 + [anywhere] * 3,
        out_specs=[pl.BlockSpec(memory_space=pltpu.VMEM)] * 2,
        out_shape=[
            jax.ShapeDtypeStruct((4, 256, 512), BF),
            jax.ShapeDtypeStruct((2, 8, 512, 512), BF),
        ],
        scratch_shapes=[
            pltpu.VMEM((2, 8, 32, 16, 128), BF),
            pltpu.VMEM((2, 1024, 256), BF),
            pltpu.VMEM((2, 512, 256), BF),
            pltpu.VMEM((2, 256, 512), BF),
            pltpu.VMEM((8, 16, 16, 128), BF),
            pltpu.VMEM((16, 8, 16, 128), BF),
            pltpu.VMEM((8, 16, 16, 128), BF),
            pltpu.VMEM((16, 8, 16, 128), BF),
            pltpu.VMEM((8, 16, 2, 16, 128), BF),
            pltpu.VMEM((2, 4, 512, 128), BF),
            pltpu.VMEM((2, 512, 512), F32),
            pltpu.SemaphoreType.DMA((2, 8)),
            pltpu.SemaphoreType.DMA((2,)),
            pltpu.SemaphoreType.DMA,
            pltpu.SemaphoreType.DMA((4,)),
            pltpu.SemaphoreType.DMA((4,)),
            pltpu.SemaphoreType.DMA((2, 8)),
            pltpu.SemaphoreType.DMA((2, 8)),
        ],
        compiler_params=pltpu.CompilerParams(
            collective_id=0, has_side_effects=True, vmem_limit_bytes=26 << 20
        ),
        cost_estimate=pl.CostEstimate(
            flops=2**30, bytes_accessed=4 << 20, transcendentals=0
        ),
        name="transform",
    )(*far)
    return pl.pallas_call(
        coupling_kernel,
        grid=(2, 4),
        in_specs=[
            pl.BlockSpec((1, 2, 512, 512), lambda o, pair: (o, pair, 0, 0)),
            pl.BlockSpec((4, 256, 512), lambda o, pair: (0, 0, 0)),
        ],
        out_specs=pl.BlockSpec(
            (1, 2, 2, 256, 2, 256), lambda o, pair: (o, 0, pair, 0, 0, 0)
        ),
        out_shape=jax.ShapeDtypeStruct((2, 2, 8, 256, 2, 256), BF),
        cost_estimate=pl.CostEstimate(
            flops=2**32, bytes_accessed=10 << 20, transcendentals=0
        ),
        compiler_params=pltpu.CompilerParams(vmem_limit_bytes=26 << 20),
        name="coupling",
    )(left, spectra)


def solution(mesh):
    return jax.shard_map(
        shards,
        mesh=mesh,
        in_specs=(P("tm", "lat", None), P(("tm", "lat"), None, None), P(), P()),
        out_specs=P(("tm", "lat"), None, None, None, None, None),
        check_vma=False,
    )
```

```python
import math

import jax
import jax.numpy as jnp
import numpy as np
from jax import lax
from jax.experimental import pallas as pl
from jax.experimental.pallas import tpu as pltpu
from jax.sharding import PartitionSpec as P

BF = jnp.bfloat16
F32 = jnp.float32


def longitude_table():
    group, op, slot = np.meshgrid(
        np.arange(4), np.arange(4), np.arange(32), indexing="ij"
    )
    order = (2 * (32 * group + slot) + op // 2).reshape(-1)
    part = (op % 2).reshape(-1)
    phase = np.arange(1024)[:, None] * order[None, :] % 1024
    angle = phase * (2.0 * math.pi / 1024)
    table = np.where(part[None, :] == 0, np.cos(angle), -np.sin(angle))
    return jnp.asarray((table / 32.0).astype(np.float32)).astype(BF)


def farthest_first(count, fields):
    def hops(i):
        return sum((0, 1, 2, 1)[i >> shift & 3] for shift in fields)

    return sorted(range(1, count), key=lambda i: (-hops(i), i))


UP = farthest_first(8, (1,))
ACROSS = farthest_first(16, (0, 2))


def swap_index_and_lanes(values, unit):
    values = list(values)
    lane = lax.broadcasted_iota(jnp.int32, values[0].shape, 1)
    step = len(values) // 2
    while step:
        low = (lane & (step * unit)) == 0
        for i in range(len(values)):
            if i & step == 0:
                a, b = values[i], values[i + step]
                values[i] = jnp.where(low, a, pltpu.roll(b, step * unit, 1))
                values[i + step] = jnp.where(
                    low, pltpu.roll(a, 128 - step * unit, 1), b
                )
        step //= 2
    return values


def transform_kernel(
    range_ref,
    offsets_ref,
    x_hbm,
    table_hbm,
    proj_hbm,
    out_ref,
    h_ref,
    left_ref,
    x_ref,
    table_ref,
    proj_ref,
    flip_ref,
    up_ref,
    across_ref,
    via_up_ref,
    via_across_ref,
    r_ref,
    a_ref,
    twice_ref,
    x_sem,
    table_sem,
    proj_sem,
    send_sem,
    recv_sem,
    pass_send_sem,
    pass_recv_sem,
):
    tm, lat = lax.axis_index("tm"), lax.axis_index("lat")
    me = 16 * tm + lat

    x_copies, table_copies = [], []
    for bh in range(2):
        for j in range(8):
            x_copies.append(
                pltpu.make_async_copy(
                    x_hbm.at[:, pl.ds(16 * bh, 16), pl.ds(128 * j, 128)],
                    x_ref.at[bh, j],
                    x_sem.at[bh, j],
                )
            )
    for j in range(2):
        table_copies.append(
            pltpu.make_async_copy(
                table_hbm.at[:, pl.ds(256 * j, 256)], table_ref.at[j], table_sem.at[j]
            )
        )
    proj_copy = pltpu.make_async_copy(proj_hbm, proj_ref, proj_sem)
    table_copies[0].start()
    for copy in x_copies[:8]:
        copy.start()
    table_copies[1].start()
    for copy in x_copies[8:]:
        copy.start()
    proj_copy.start()

    barrier = pltpu.get_barrier_semaphore()
    for i in range(1, 8):
        pl.semaphore_signal(barrier, inc=1, device_id=(tm ^ i, lat))
    for i in range(1, 16):
        pl.semaphore_signal(barrier, inc=1, device_id=(tm, lat ^ i))

    @pl.when((lat == 0) & (tm > 0))
    def _():
        pl.semaphore_signal(barrier, inc=1, device_id=(tm - 1, 15))

    @pl.when((lat == 15) & (tm < 7))
    def _():
        pl.semaphore_signal(barrier, inc=1, device_id=(tm + 1, 0))

    outside = ((lat == 0) & (tm > 0)) | ((lat == 15) & (tm < 7))

    def up(i, source, target, stage):
        return pltpu.make_async_remote_copy(
            src_ref=source,
            dst_ref=target,
            send_sem=send_sem.at[stage],
            recv_sem=recv_sem.at[stage],
            device_id=(tm ^ i, lat),
        )

    def across(i, source, target, stage):
        return pltpu.make_async_remote_copy(
            src_ref=source,
            dst_ref=target,
            send_sem=send_sem.at[stage],
            recv_sem=recv_sem.at[stage],
            device_id=(tm, lat ^ i),
        )

    for bh in range(2):
        for copy in x_copies[8 * bh : 8 * bh + 8]:
            copy.wait()
        for gp in range(2):
            if bh == 0:
                table_copies[gp].wait()
            x = jnp.concatenate(
                [x_ref[bh, j].reshape(512, 128) for j in range(8)], axis=1
            )
            z = jnp.dot(x, table_ref[gp], preferred_element_type=F32)
            z = z.astype(BF).reshape(32, 16, 256)
            for c in range(2):
                v = [z[t, :, 128 * c : 128 * c + 128] for t in range(32)]
                v = swap_index_and_lanes(v, 1)
                for slot in range(32):
                    to_tm, to_lat = 2 * (2 * gp + c) + slot // 16, slot % 16
                    if bh == 0:
                        up_ref[to_tm, to_lat] = v[slot]
                    else:
                        across_ref[to_lat, to_tm] = v[slot]
    pl.semaphore_wait(barrier, 22 + outside.astype(jnp.int32))
    for i in ACROSS[:8]:
        across(i, across_ref.at[lat ^ i], via_across_ref.at[lat], 1).start()
    for i in UP:
        up(i, up_ref.at[tm ^ i], via_up_ref.at[tm], 0).start()
    for i in ACROSS[8:]:
        across(i, across_ref.at[lat ^ i], via_across_ref.at[lat], 1).start()
    via_up_ref[tm] = up_ref[tm]
    via_across_ref[lat] = across_ref[lat]

    proj_copy.wait()
    for o in range(2):
        flip_ref[o] = proj_ref[o].T

    some = pl.ds(0, 7)
    up_all = up(0, up_ref.at[some], via_up_ref.at[some], 0)
    up_all.wait_recv()
    for i in ACROSS:
        across(i, via_up_ref.at[:, lat ^ i], r_ref.at[:, lat, 0], 2).start()
    some = pl.ds(0, 15)
    across_all = across(0, across_ref.at[some], via_across_ref.at[some], 1)
    across_all.wait_recv()
    for i in UP:
        up(i, via_across_ref.at[:, tm ^ i], r_ref.at[tm, :, 1], 3).start()
    r_ref[:, lat, 0] = via_up_ref[:, lat]
    r_ref[tm, :, 1] = via_across_ref[:, tm]

    across_last = across(
        0, via_across_ref.at[pl.ds(0, 15)], r_ref.at[:, pl.ds(0, 15), 0], 2
    )
    up_last = up(0, via_up_ref.at[pl.ds(0, 7)], r_ref.at[pl.ds(0, 7), :, 1], 3)
    for half in range(2):
        if half == 0:
            across_last.wait_recv()
        else:
            up_last.wait_recv()
        for i in range(16):
            rows = slice(32 * i + 16 * half, 32 * i + 16 * half + 16)
            for q in range(2):
                v = [r_ref[4 * q + j, i, half] for j in range(4)]
                v = swap_index_and_lanes(v, 32)
                for op in range(4):
                    a_ref[op // 2, 2 * (op % 2) + q, rows, :] = v[op]
    degree = lax.broadcasted_iota(jnp.int32, (256, 512), 0)
    before = jnp.maximum(me - 1, 0)

    def passed(o, c):
        rows = pl.ds(32 * c, 32)
        return pltpu.make_async_remote_copy(
            src_ref=h_ref.at[o, rows],
            dst_ref=h_ref.at[2 + o, rows],
            send_sem=pass_send_sem.at[o, c],
            recv_sem=pass_recv_sem.at[o, c],
            device_id=(before >> 4, before & 15),
        )

    for o in range(2):
        columns = jnp.concatenate([a_ref[o, j] for j in range(4)], axis=1)
        h = jnp.dot(flip_ref[o], columns, preferred_element_type=F32)
        low, high = range_ref[0, 2 * me + o], range_ref[1, 2 * me + o]
        keep = (degree >= low) & (degree < high)
        h_ref[o] = jnp.where(keep, h, 0.0).astype(BF)
        for c in range(8):

            @pl.when((me > 0) & (32 * (c + 1) > 2 * me + o))
            def _():
                passed(o, c).start()

    up_all.wait_send()
    across_all.wait_send()
    across_last.wait_send()
    up_last.wait_send()

    row = lax.broadcasted_iota(jnp.int32, (512, 256), 0)
    column = lax.broadcasted_iota(jnp.int32, (512, 256), 1)
    double = ((row >> 1) == column).astype(F32).astype(BF)
    for o in range(2):
        twice_ref[o] = jnp.dot(double, h_ref[o], preferred_element_type=F32)

    @pl.loop(0, 8)
    def _(k):
        cos, sin = phases(offsets_ref[k])
        cos = jnp.broadcast_to(cos[None], (64, 8, 256)).reshape(512, 256)
        sin = jnp.broadcast_to(sin[None], (64, 8, 256)).reshape(512, 256)
        for o in range(2):
            real, imag = twice_ref[o, :, :256], twice_ref[o, :, 256:]
            left_ref[o, k, :, :256] = (real * cos - imag * sin).astype(BF)
            left_ref[o, k, :, 256:] = (real * sin + imag * cos).astype(BF)

    def couple(o, s):
        @pl.loop(0, 2)
        def _(half):
            for i in range(4):
                product = lax.dot_general(
                    left_ref[o, 4 * half + i],
                    h_ref[o + 1 + s],
                    (((1,), (1,)), ((), ())),
                    preferred_element_type=F32,
                )
                out_ref[o, s, 4 * half + i] = product.astype(BF).reshape(256, 2, 256)

    def receive(o):
        for c in range(8):
            sent = (me < 127) & (32 * (c + 1) > 2 * (me + 1) + o)

            @pl.when(sent)
            def _():
                passed(o, c).wait_recv()

            @pl.when(jnp.logical_not(sent))
            def _():
                h_ref[2 + o, 32 * c : 32 * c + 32] = jnp.zeros((32, 512), BF)

    couple(0, 0)
    receive(0)
    couple(0, 1)
    couple(1, 0)
    receive(1)
    couple(1, 1)
    for o in range(2):
        for c in range(8):

            @pl.when((me > 0) & (32 * (c + 1) > 2 * me + o))
            def _():
                passed(o, c).wait_send()


def phases(offset):
    row = lax.broadcasted_iota(jnp.int32, (8, 256), 0)
    t = lax.broadcasted_iota(jnp.int32, (8, 256), 1)
    turn = (offset * t + 64 * (row & 1)) & 255
    angle = turn.astype(F32) * (2.0 * math.pi / 256)
    return jnp.cos(angle) * (1.0 / 16), jnp.sin(angle) * (1.0 / 16)


def shards(frames, projection, degree_range, offsets):
    anywhere = pl.BlockSpec(memory_space=pltpu.HBM)
    far = [
        pltpu.with_memory_space_constraint(a, pltpu.HBM)
        for a in (degree_range.T, offsets, frames, longitude_table(), projection)
    ]
    return pl.pallas_call(
        transform_kernel,
        in_specs=[pl.BlockSpec(memory_space=pltpu.SMEM)] * 2 + [anywhere] * 3,
        out_specs=pl.BlockSpec(memory_space=pltpu.VMEM),
        out_shape=jax.ShapeDtypeStruct((2, 2, 8, 256, 2, 256), BF),
        scratch_shapes=[
            pltpu.VMEM((4, 256, 512), BF),
            pltpu.VMEM((2, 8, 512, 512), BF),
            pltpu.VMEM((2, 8, 32, 16, 128), BF),
            pltpu.VMEM((2, 1024, 256), BF),
            pltpu.VMEM((2, 512, 256), BF),
            pltpu.VMEM((2, 256, 512), BF),
            pltpu.VMEM((8, 16, 16, 128), BF),
            pltpu.VMEM((16, 8, 16, 128), BF),
            pltpu.VMEM((8, 16, 16, 128), BF),
            pltpu.VMEM((16, 8, 16, 128), BF),
            pltpu.VMEM((8, 16, 2, 16, 128), BF),
            pltpu.VMEM((2, 4, 512, 128), BF),
            pltpu.VMEM((2, 512, 512), F32),
            pltpu.SemaphoreType.DMA((2, 8)),
            pltpu.SemaphoreType.DMA((2,)),
            pltpu.SemaphoreType.DMA,
            pltpu.SemaphoreType.DMA((4,)),
            pltpu.SemaphoreType.DMA((4,)),
            pltpu.SemaphoreType.DMA((2, 8)),
            pltpu.SemaphoreType.DMA((2, 8)),
        ],
        compiler_params=pltpu.CompilerParams(
            collective_id=0, has_side_effects=True, vmem_limit_bytes=36 << 20
        ),
        cost_estimate=pl.CostEstimate(
            flops=2**32, bytes_accessed=12 << 20, transcendentals=0
        ),
        name="transform",
    )(*far)


def solution(mesh):
    return jax.shard_map(
        shards,
        mesh=mesh,
        in_specs=(P("tm", "lat", None), P(("tm", "lat"), None, None), P(), P()),
        out_specs=P(("tm", "lat"), None, None, None, None, None),
        check_vma=False,
    )
```

```python
import math

import jax
import jax.numpy as jnp
import numpy as np
from jax import lax
from jax.experimental import pallas as pl
from jax.experimental.pallas import tpu as pltpu
from jax.sharding import PartitionSpec as P

BF = jnp.bfloat16
F32 = jnp.float32


def longitude_table():
    group, op, slot = np.meshgrid(
        np.arange(4), np.arange(4), np.arange(32), indexing="ij"
    )
    order = (2 * (32 * group + slot) + op // 2).reshape(-1)
    part = (op % 2).reshape(-1)
    phase = np.arange(1024)[:, None] * order[None, :] % 1024
    angle = phase * (2.0 * math.pi / 1024)
    table = np.where(part[None, :] == 0, np.cos(angle), -np.sin(angle))
    return jnp.asarray((table / 32.0).astype(np.float32)).astype(BF)


def farthest_first(count, fields):
    def hops(i):
        return sum((0, 1, 2, 1)[i >> shift & 3] for shift in fields)

    return sorted(range(1, count), key=lambda i: (-hops(i), i))


UP = farthest_first(8, (1,))
ACROSS = farthest_first(16, (0, 2))


def swap_index_and_lanes(values, unit):
    values = list(values)
    lane = lax.broadcasted_iota(jnp.int32, values[0].shape, 1)
    step = len(values) // 2
    while step:
        low = (lane & (step * unit)) == 0
        for i in range(len(values)):
            if i & step == 0:
                a, b = values[i], values[i + step]
                values[i] = jnp.where(low, a, pltpu.roll(b, step * unit, 1))
                values[i + step] = jnp.where(
                    low, pltpu.roll(a, 128 - step * unit, 1), b
                )
        step //= 2
    return values


def transform_kernel(
    range_ref,
    offsets_ref,
    x_hbm,
    table_hbm,
    proj_hbm,
    out_ref,
    last_ref,
    left_ref,
    h_ref,
    left0_ref,
    x_ref,
    table_ref,
    proj_ref,
    flip_ref,
    up_ref,
    across_ref,
    via_up_ref,
    via_across_ref,
    r_ref,
    a_ref,
    twice_ref,
    x_sem,
    table_sem,
    proj_sem,
    send_sem,
    recv_sem,
    pass_send_sem,
    pass_recv_sem,
):
    tm, lat = lax.axis_index("tm"), lax.axis_index("lat")
    me = 16 * tm + lat

    x_copies, table_copies = [], []
    for bh in range(2):
        for j in range(8):
            x_copies.append(
                pltpu.make_async_copy(
                    x_hbm.at[:, pl.ds(16 * bh, 16), pl.ds(128 * j, 128)],
                    x_ref.at[bh, j],
                    x_sem.at[bh, j],
                )
            )
    for j in range(2):
        table_copies.append(
            pltpu.make_async_copy(
                table_hbm.at[:, pl.ds(256 * j, 256)], table_ref.at[j], table_sem.at[j]
            )
        )
    proj_copy = pltpu.make_async_copy(proj_hbm, proj_ref, proj_sem)
    table_copies[0].start()
    for copy in x_copies[:8]:
        copy.start()
    table_copies[1].start()
    for copy in x_copies[8:]:
        copy.start()
    proj_copy.start()

    barrier = pltpu.get_barrier_semaphore()
    for i in range(1, 8):
        pl.semaphore_signal(barrier, inc=1, device_id=(tm ^ i, lat))
    for i in range(1, 16):
        pl.semaphore_signal(barrier, inc=1, device_id=(tm, lat ^ i))

    @pl.when((lat == 0) & (tm > 0))
    def _():
        pl.semaphore_signal(barrier, inc=1, device_id=(tm - 1, 15))

    @pl.when((lat == 15) & (tm < 7))
    def _():
        pl.semaphore_signal(barrier, inc=1, device_id=(tm + 1, 0))

    outside = ((lat == 0) & (tm > 0)) | ((lat == 15) & (tm < 7))

    def up(i, source, target, stage):
        return pltpu.make_async_remote_copy(
            src_ref=source,
            dst_ref=target,
            send_sem=send_sem.at[stage],
            recv_sem=recv_sem.at[stage],
            device_id=(tm ^ i, lat),
        )

    def across(i, source, target, stage):
        return pltpu.make_async_remote_copy(
            src_ref=source,
            dst_ref=target,
            send_sem=send_sem.at[stage],
            recv_sem=recv_sem.at[stage],
            device_id=(tm, lat ^ i),
        )

    for bh in range(2):
        for copy in x_copies[8 * bh : 8 * bh + 8]:
            copy.wait()
        for gp in range(2):
            if bh == 0:
                table_copies[gp].wait()
            x = jnp.concatenate(
                [x_ref[bh, j].reshape(512, 128) for j in range(8)], axis=1
            )
            z = jnp.dot(x, table_ref[gp], preferred_element_type=F32)
            z = z.astype(BF).reshape(32, 16, 256)
            for c in range(2):
                v = [z[t, :, 128 * c : 128 * c + 128] for t in range(32)]
                v = swap_index_and_lanes(v, 1)
                for slot in range(32):
                    to_tm, to_lat = 2 * (2 * gp + c) + slot // 16, slot % 16
                    if bh == 0:
                        up_ref[to_tm, to_lat] = v[slot]
                    else:
                        across_ref[to_lat, to_tm] = v[slot]
    pl.semaphore_wait(barrier, 22 + outside.astype(jnp.int32))
    for i in ACROSS[:8]:
        across(i, across_ref.at[lat ^ i], via_across_ref.at[lat], 1).start()
    for i in UP:
        up(i, up_ref.at[tm ^ i], via_up_ref.at[tm], 0).start()
    for i in ACROSS[8:]:
        across(i, across_ref.at[lat ^ i], via_across_ref.at[lat], 1).start()
    via_up_ref[tm] = up_ref[tm]
    via_across_ref[lat] = across_ref[lat]

    proj_copy.wait()
    for o in range(2):
        flip_ref[o] = proj_ref[o].T

    some = pl.ds(0, 7)
    up_all = up(0, up_ref.at[some], via_up_ref.at[some], 0)
    up_all.wait_recv()
    for i in ACROSS:
        across(i, via_up_ref.at[:, lat ^ i], r_ref.at[:, lat, 0], 2).start()
    some = pl.ds(0, 15)
    across_all = across(0, across_ref.at[some], via_across_ref.at[some], 1)
    across_all.wait_recv()
    for i in UP:
        up(i, via_across_ref.at[:, tm ^ i], r_ref.at[tm, :, 1], 3).start()
    r_ref[:, lat, 0] = via_up_ref[:, lat]
    r_ref[tm, :, 1] = via_across_ref[:, tm]

    across_last = across(
        0, via_across_ref.at[pl.ds(0, 15)], r_ref.at[:, pl.ds(0, 15), 0], 2
    )
    up_last = up(0, via_up_ref.at[pl.ds(0, 7)], r_ref.at[pl.ds(0, 7), :, 1], 3)
    for half in range(2):
        if half == 0:
            across_last.wait_recv()
        else:
            up_last.wait_recv()
        for i in range(16):
            rows = slice(32 * i + 16 * half, 32 * i + 16 * half + 16)
            for q in range(2):
                v = [r_ref[4 * q + j, i, half] for j in range(4)]
                v = swap_index_and_lanes(v, 32)
                for op in range(4):
                    a_ref[op // 2, 2 * (op % 2) + q, rows, :] = v[op]
    degree = lax.broadcasted_iota(jnp.int32, (256, 512), 0)
    before = jnp.maximum(me - 1, 0)

    def passed(o, c):
        rows = pl.ds(32 * c, 32)
        return pltpu.make_async_remote_copy(
            src_ref=h_ref.at[o, rows],
            dst_ref=h_ref.at[2 + o, rows],
            send_sem=pass_send_sem.at[o, c],
            recv_sem=pass_recv_sem.at[o, c],
            device_id=(before >> 4, before & 15),
        )

    for o in range(2):
        columns = jnp.concatenate([a_ref[o, j] for j in range(4)], axis=1)
        h = jnp.dot(flip_ref[o], columns, preferred_element_type=F32)
        low, high = range_ref[0, 2 * me + o], range_ref[1, 2 * me + o]
        keep = (degree >= low) & (degree < high)
        h_ref[o] = jnp.where(keep, h, 0.0).astype(BF)
        for c in range(8):

            @pl.when((me > 0) & (32 * (c + 1) > 2 * me + o))
            def _():
                passed(o, c).start()

    up_all.wait_send()
    across_all.wait_send()
    across_last.wait_send()
    up_last.wait_send()

    row = lax.broadcasted_iota(jnp.int32, (512, 256), 0)
    column = lax.broadcasted_iota(jnp.int32, (512, 256), 1)
    double = ((row >> 1) == column).astype(F32).astype(BF)
    for o in range(2):
        twice_ref[o] = jnp.dot(double, h_ref[o], preferred_element_type=F32)

    def build(o, k, target):
        cos, sin = phases(offsets_ref[k])
        cos = jnp.broadcast_to(cos[None], (64, 8, 256)).reshape(512, 256)
        sin = jnp.broadcast_to(sin[None], (64, 8, 256)).reshape(512, 256)
        real, imag = twice_ref[o, :, :256], twice_ref[o, :, 256:]
        target[k, :, :256] = (real * cos - imag * sin).astype(BF)
        target[k, :, 256:] = (real * sin + imag * cos).astype(BF)

    @pl.loop(0, 8)
    def _(k):
        build(0, k, left0_ref)

    def couple(place, left, partner, with_build=False):
        @pl.loop(0, 2)
        def _(half):
            for i in range(4):
                if with_build:
                    build(1, 4 * half + i, left_ref)
                product = lax.dot_general(
                    left[4 * half + i],
                    h_ref[partner],
                    (((1,), (1,)), ((), ())),
                    preferred_element_type=F32,
                )
                out_ref[place, 4 * half + i] = product.astype(BF).reshape(256, 2, 256)

    def receive(o):
        for c in range(8):
            sent = (me < 127) & (32 * (c + 1) > 2 * (me + 1) + o)

            @pl.when(sent)
            def _():
                passed(o, c).wait_recv()

            @pl.when(jnp.logical_not(sent))
            def _():
                h_ref[2 + o, 32 * c : 32 * c + 32] = jnp.zeros((32, 512), BF)

    couple(0, left0_ref, 1, with_build=True)
    receive(0)
    couple(1, left0_ref, 2)
    couple(2, left_ref, 2)
    receive(1)
    last_ref[...] = h_ref[3]
    for o in range(2):
        for c in range(8):

            @pl.when((me > 0) & (32 * (c + 1) > 2 * me + o))
            def _():
                passed(o, c).wait_send()


def phases(offset):
    row = lax.broadcasted_iota(jnp.int32, (8, 256), 0)
    t = lax.broadcasted_iota(jnp.int32, (8, 256), 1)
    turn = (offset * t + 64 * (row & 1)) & 255
    angle = turn.astype(F32) * (2.0 * math.pi / 256)
    return jnp.cos(angle) * (1.0 / 16), jnp.sin(angle) * (1.0 / 16)


def finish_kernel(out_ref, last_ref, left_ref, out_hbm, block_ref, early_sem, late_sem):
    early = [
        pltpu.make_async_copy(out_ref.at[i], out_hbm.at[o, s], early_sem.at[i])
        for i, (o, s) in enumerate(((0, 0), (0, 1), (1, 0)))
    ]
    for copy in early:
        copy.start()

    def late(half):
        some = pl.ds(4 * half, 4)
        return pltpu.make_async_copy(
            block_ref.at[some], out_hbm.at[1, 1, some], late_sem.at[half]
        )

    @pl.loop(0, 2)
    def _(half):
        for i in range(4):
            product = lax.dot_general(
                left_ref[4 * half + i],
                last_ref[...],
                (((1,), (1,)), ((), ())),
                preferred_element_type=F32,
            )
            block_ref[4 * half + i] = product.astype(BF).reshape(256, 2, 256)
        late(half).start()

    for copy in early:
        copy.wait()
    for half in range(2):
        late(half).wait()


def shards(frames, projection, degree_range, offsets):
    anywhere = pl.BlockSpec(memory_space=pltpu.HBM)
    far = [
        pltpu.with_memory_space_constraint(a, pltpu.HBM)
        for a in (degree_range.T, offsets, frames, longitude_table(), projection)
    ]
    ready, last, left = pl.pallas_call(
        transform_kernel,
        in_specs=[pl.BlockSpec(memory_space=pltpu.SMEM)] * 2 + [anywhere] * 3,
        out_specs=[pl.BlockSpec(memory_space=pltpu.VMEM)] * 3,
        out_shape=[
            jax.ShapeDtypeStruct((3, 8, 256, 2, 256), BF),
            jax.ShapeDtypeStruct((256, 512), BF),
            jax.ShapeDtypeStruct((8, 512, 512), BF),
        ],
        scratch_shapes=[
            pltpu.VMEM((4, 256, 512), BF),
            pltpu.VMEM((8, 512, 512), BF),
            pltpu.VMEM((2, 8, 32, 16, 128), BF),
            pltpu.VMEM((2, 1024, 256), BF),
            pltpu.VMEM((2, 512, 256), BF),
            pltpu.VMEM((2, 256, 512), BF),
            pltpu.VMEM((8, 16, 16, 128), BF),
            pltpu.VMEM((16, 8, 16, 128), BF),
            pltpu.VMEM((8, 16, 16, 128), BF),
            pltpu.VMEM((16, 8, 16, 128), BF),
            pltpu.VMEM((8, 16, 2, 16, 128), BF),
            pltpu.VMEM((2, 4, 512, 128), BF),
            pltpu.VMEM((2, 512, 512), F32),
            pltpu.SemaphoreType.DMA((2, 8)),
            pltpu.SemaphoreType.DMA((2,)),
            pltpu.SemaphoreType.DMA,
            pltpu.SemaphoreType.DMA((4,)),
            pltpu.SemaphoreType.DMA((4,)),
            pltpu.SemaphoreType.DMA((2, 8)),
            pltpu.SemaphoreType.DMA((2, 8)),
        ],
        compiler_params=pltpu.CompilerParams(
            collective_id=0, has_side_effects=True, vmem_limit_bytes=36 << 20
        ),
        cost_estimate=pl.CostEstimate(
            flops=2**32, bytes_accessed=12 << 20, transcendentals=0
        ),
        name="transform",
    )(*far)
    return pl.pallas_call(
        finish_kernel,
        in_specs=[pl.BlockSpec(memory_space=pltpu.VMEM)] * 3,
        out_specs=anywhere,
        out_shape=jax.ShapeDtypeStruct((2, 2, 8, 256, 2, 256), BF),
        scratch_shapes=[
            pltpu.VMEM((8, 256, 2, 256), BF),
            pltpu.SemaphoreType.DMA((3,)),
            pltpu.SemaphoreType.DMA((2,)),
        ],
        compiler_params=pltpu.CompilerParams(vmem_limit_bytes=26 << 20),
        cost_estimate=pl.CostEstimate(
            flops=2**30, bytes_accessed=8 << 20, transcendentals=0
        ),
        name="finish",
    )(ready, last, left)


def solution(mesh):
    return jax.shard_map(
        shards,
        mesh=mesh,
        in_specs=(P("tm", "lat", None), P(("tm", "lat"), None, None), P(), P()),
        out_specs=P(("tm", "lat"), None, None, None, None, None),
        check_vma=False,
    )
```

```python
import math

import jax
import jax.numpy as jnp
import numpy as np
from jax import lax
from jax.experimental import pallas as pl
from jax.experimental.pallas import tpu as pltpu
from jax.sharding import PartitionSpec as P

BF = jnp.bfloat16
F32 = jnp.float32


def longitude_table():
    group, op, slot = np.meshgrid(
        np.arange(4), np.arange(4), np.arange(32), indexing="ij"
    )
    order = (2 * (32 * group + slot) + op // 2).reshape(-1)
    part = (op % 2).reshape(-1)
    phase = np.arange(1024)[:, None] * order[None, :] % 1024
    angle = phase * (2.0 * math.pi / 1024)
    table = np.where(part[None, :] == 0, np.cos(angle), -np.sin(angle))
    return jnp.asarray((table / 32.0).astype(np.float32)).astype(BF)


def farthest_first(count, fields):
    def hops(i):
        return sum((0, 1, 2, 1)[i >> shift & 3] for shift in fields)

    return sorted(range(1, count), key=lambda i: (-hops(i), i))


UP = farthest_first(8, (1,))
ACROSS = farthest_first(16, (0, 2))


def swap_index_and_lanes(values, unit):
    values = list(values)
    lane = lax.broadcasted_iota(jnp.int32, values[0].shape, 1)
    step = len(values) // 2
    while step:
        low = (lane & (step * unit)) == 0
        for i in range(len(values)):
            if i & step == 0:
                a, b = values[i], values[i + step]
                values[i] = jnp.where(low, a, pltpu.roll(b, step * unit, 1))
                values[i + step] = jnp.where(
                    low, pltpu.roll(a, 128 - step * unit, 1), b
                )
        step //= 2
    return values


def transform_kernel(
    range_ref,
    offsets_ref,
    x_hbm,
    table_hbm,
    proj_hbm,
    out_ref,
    last_ref,
    left_ref,
    h_ref,
    left0_ref,
    x_ref,
    table_ref,
    proj_ref,
    flip_ref,
    up_ref,
    across_ref,
    via_up_ref,
    via_across_ref,
    r_ref,
    a_ref,
    twice_ref,
    x_sem,
    table_sem,
    proj_sem,
    send_sem,
    recv_sem,
    pass_send_sem,
    pass_recv_sem,
):
    tm, lat = lax.axis_index("tm"), lax.axis_index("lat")
    me = 16 * tm + lat

    x_copies, table_copies = [], []
    for bh in range(2):
        for j in range(8):
            x_copies.append(
                pltpu.make_async_copy(
                    x_hbm.at[:, pl.ds(16 * bh, 16), pl.ds(128 * j, 128)],
                    x_ref.at[bh, j],
                    x_sem.at[bh, j],
                )
            )
    for j in range(2):
        table_copies.append(
            pltpu.make_async_copy(
                table_hbm.at[:, pl.ds(256 * j, 256)], table_ref.at[j], table_sem.at[j]
            )
        )
    proj_copy = pltpu.make_async_copy(proj_hbm, proj_ref, proj_sem)
    table_copies[0].start()
    for copy in x_copies[:8]:
        copy.start()
    table_copies[1].start()
    for copy in x_copies[8:]:
        copy.start()
    proj_copy.start()

    barrier = pltpu.get_barrier_semaphore()
    for i in range(1, 8):
        pl.semaphore_signal(barrier, inc=1, device_id=(tm ^ i, lat))
    for i in range(1, 16):
        pl.semaphore_signal(barrier, inc=1, device_id=(tm, lat ^ i))

    @pl.when((lat == 0) & (tm > 0))
    def _():
        pl.semaphore_signal(barrier, inc=1, device_id=(tm - 1, 15))

    @pl.when((lat == 15) & (tm < 7))
    def _():
        pl.semaphore_signal(barrier, inc=1, device_id=(tm + 1, 0))

    outside = ((lat == 0) & (tm > 0)) | ((lat == 15) & (tm < 7))

    def up(i, source, target, stage):
        return pltpu.make_async_remote_copy(
            src_ref=source,
            dst_ref=target,
            send_sem=send_sem.at[stage],
            recv_sem=recv_sem.at[stage],
            device_id=(tm ^ i, lat),
        )

    def across(i, source, target, stage):
        return pltpu.make_async_remote_copy(
            src_ref=source,
            dst_ref=target,
            send_sem=send_sem.at[stage],
            recv_sem=recv_sem.at[stage],
            device_id=(tm, lat ^ i),
        )

    for bh in range(2):
        for copy in x_copies[8 * bh : 8 * bh + 8]:
            copy.wait()
        for gp in range(2):
            if bh == 0:
                table_copies[gp].wait()
            x = jnp.concatenate(
                [x_ref[bh, j].reshape(512, 128) for j in range(8)], axis=1
            )
            z = jnp.dot(x, table_ref[gp], preferred_element_type=F32)
            z = z.astype(BF).reshape(32, 16, 256)
            for c in range(2):
                v = [z[t, :, 128 * c : 128 * c + 128] for t in range(32)]
                v = swap_index_and_lanes(v, 1)
                for slot in range(32):
                    to_tm, to_lat = 2 * (2 * gp + c) + slot // 16, slot % 16
                    if bh == 0:
                        up_ref[to_tm, to_lat] = v[slot]
                    else:
                        across_ref[to_lat, to_tm] = v[slot]
        if bh == 0:
            pl.semaphore_wait(barrier, 22 + outside.astype(jnp.int32))
            for i in UP:
                up(i, up_ref.at[tm ^ i], via_up_ref.at[tm], 0).start()

    for i in ACROSS:
        across(i, across_ref.at[lat ^ i], via_across_ref.at[lat], 1).start()
    via_up_ref[tm] = up_ref[tm]
    via_across_ref[lat] = across_ref[lat]

    proj_copy.wait()
    for o in range(2):
        flip_ref[o] = proj_ref[o].T

    some = pl.ds(0, 7)
    up_all = up(0, up_ref.at[some], via_up_ref.at[some], 0)
    up_all.wait_recv()
    for i in ACROSS:
        across(i, via_up_ref.at[:, lat ^ i], r_ref.at[:, lat, 0], 2).start()
    some = pl.ds(0, 15)
    across_all = across(0, across_ref.at[some], via_across_ref.at[some], 1)
    across_all.wait_recv()
    for i in UP:
        up(i, via_across_ref.at[:, tm ^ i], r_ref.at[tm, :, 1], 3).start()
    r_ref[:, lat, 0] = via_up_ref[:, lat]
    r_ref[tm, :, 1] = via_across_ref[:, tm]

    across_last = across(
        0, via_across_ref.at[pl.ds(0, 15)], r_ref.at[:, pl.ds(0, 15), 0], 2
    )
    up_last = up(0, via_up_ref.at[pl.ds(0, 7)], r_ref.at[pl.ds(0, 7), :, 1], 3)
    for half in range(2):
        if half == 0:
            across_last.wait_recv()
        else:
            up_last.wait_recv()
        for i in range(16):
            rows = slice(32 * i + 16 * half, 32 * i + 16 * half + 16)
            for q in range(2):
                v = [r_ref[4 * q + j, i, half] for j in range(4)]
                v = swap_index_and_lanes(v, 32)
                for op in range(4):
                    a_ref[op // 2, 2 * (op % 2) + q, rows, :] = v[op]
    degree = lax.broadcasted_iota(jnp.int32, (256, 512), 0)
    before = jnp.maximum(me - 1, 0)

    def passed(o, c):
        rows = pl.ds(32 * c, 32)
        return pltpu.make_async_remote_copy(
            src_ref=h_ref.at[o, rows],
            dst_ref=h_ref.at[2 + o, rows],
            send_sem=pass_send_sem.at[o, c],
            recv_sem=pass_recv_sem.at[o, c],
            device_id=(before >> 4, before & 15),
        )

    for o in range(2):
        columns = jnp.concatenate([a_ref[o, j] for j in range(4)], axis=1)
        h = jnp.dot(flip_ref[o], columns, preferred_element_type=F32)
        low, high = range_ref[0, 2 * me + o], range_ref[1, 2 * me + o]
        keep = (degree >= low) & (degree < high)
        h_ref[o] = jnp.where(keep, h, 0.0).astype(BF)
        for c in range(8):

            @pl.when((me > 0) & (32 * (c + 1) > 2 * me + o))
            def _():
                passed(o, c).start()

    up_all.wait_send()
    across_all.wait_send()
    across_last.wait_send()
    up_last.wait_send()

    row = lax.broadcasted_iota(jnp.int32, (512, 256), 0)
    column = lax.broadcasted_iota(jnp.int32, (512, 256), 1)
    double = ((row >> 1) == column).astype(F32).astype(BF)
    for o in range(2):
        twice_ref[o] = jnp.dot(double, h_ref[o], preferred_element_type=F32)

    def build(o, k, target):
        cos, sin = phases(offsets_ref[k])
        cos = jnp.broadcast_to(cos[None], (64, 8, 256)).reshape(512, 256)
        sin = jnp.broadcast_to(sin[None], (64, 8, 256)).reshape(512, 256)
        real, imag = twice_ref[o, :, :256], twice_ref[o, :, 256:]
        target[k, :, :256] = (real * cos - imag * sin).astype(BF)
        target[k, :, 256:] = (real * sin + imag * cos).astype(BF)

    @pl.loop(0, 8)
    def _(k):
        build(0, k, left0_ref)

    def couple(place, left, partner, with_build=False):
        @pl.loop(0, 2)
        def _(half):
            for i in range(4):
                if with_build:
                    build(1, 4 * half + i, left_ref)
                product = lax.dot_general(
                    left[4 * half + i],
                    h_ref[partner],
                    (((1,), (1,)), ((), ())),
                    preferred_element_type=F32,
                )
                out_ref[place, 4 * half + i] = product.astype(BF).reshape(256, 2, 256)

    def receive(o):
        for c in range(8):
            sent = (me < 127) & (32 * (c + 1) > 2 * (me + 1) + o)

            @pl.when(sent)
            def _():
                passed(o, c).wait_recv()

            @pl.when(jnp.logical_not(sent))
            def _():
                h_ref[2 + o, 32 * c : 32 * c + 32] = jnp.zeros((32, 512), BF)

    couple(0, left0_ref, 1, with_build=True)
    receive(0)
    couple(1, left0_ref, 2)
    couple(2, left_ref, 2)
    receive(1)
    last_ref[...] = h_ref[3]
    for o in range(2):
        for c in range(8):

            @pl.when((me > 0) & (32 * (c + 1) > 2 * me + o))
            def _():
                passed(o, c).wait_send()


def phases(offset):
    row = lax.broadcasted_iota(jnp.int32, (8, 256), 0)
    t = lax.broadcasted_iota(jnp.int32, (8, 256), 1)
    turn = (offset * t + 64 * (row & 1)) & 255
    angle = turn.astype(F32) * (2.0 * math.pi / 256)
    return jnp.cos(angle) * (1.0 / 16), jnp.sin(angle) * (1.0 / 16)


def finish_kernel(out_ref, last_ref, left_ref, out_hbm, block_ref, early_sem, late_sem):
    early = [
        pltpu.make_async_copy(out_ref.at[i], out_hbm.at[o, s], early_sem.at[i])
        for i, (o, s) in enumerate(((0, 0), (0, 1), (1, 0)))
    ]
    for copy in early:
        copy.start()

    def late(half):
        some = pl.ds(4 * half, 4)
        return pltpu.make_async_copy(
            block_ref.at[some], out_hbm.at[1, 1, some], late_sem.at[half]
        )

    @pl.loop(0, 2)
    def _(half):
        for i in range(4):
            product = lax.dot_general(
                left_ref[4 * half + i],
                last_ref[...],
                (((1,), (1,)), ((), ())),
                preferred_element_type=F32,
            )
            block_ref[4 * half + i] = product.astype(BF).reshape(256, 2, 256)
        late(half).start()

    for copy in early:
        copy.wait()
    for half in range(2):
        late(half).wait()


def shards(frames, projection, degree_range, offsets):
    anywhere = pl.BlockSpec(memory_space=pltpu.HBM)
    far = [
        pltpu.with_memory_space_constraint(a, pltpu.HBM)
        for a in (degree_range.T, offsets, frames, longitude_table(), projection)
    ]
    ready, last, left = pl.pallas_call(
        transform_kernel,
        in_specs=[pl.BlockSpec(memory_space=pltpu.SMEM)] * 2 + [anywhere] * 3,
        out_specs=[pl.BlockSpec(memory_space=pltpu.VMEM)] * 3,
        out_shape=[
            jax.ShapeDtypeStruct((3, 8, 256, 2, 256), BF),
            jax.ShapeDtypeStruct((256, 512), BF),
            jax.ShapeDtypeStruct((8, 512, 512), BF),
        ],
        scratch_shapes=[
            pltpu.VMEM((4, 256, 512), BF),
            pltpu.VMEM((8, 512, 512), BF),
            pltpu.VMEM((2, 8, 32, 16, 128), BF),
            pltpu.VMEM((2, 1024, 256), BF),
            pltpu.VMEM((2, 512, 256), BF),
            pltpu.VMEM((2, 256, 512), BF),
            pltpu.VMEM((8, 16, 16, 128), BF),
            pltpu.VMEM((16, 8, 16, 128), BF),
            pltpu.VMEM((8, 16, 16, 128), BF),
            pltpu.VMEM((16, 8, 16, 128), BF),
            pltpu.VMEM((8, 16, 2, 16, 128), BF),
            pltpu.VMEM((2, 4, 512, 128), BF),
            pltpu.VMEM((2, 512, 512), F32),
            pltpu.SemaphoreType.DMA((2, 8)),
            pltpu.SemaphoreType.DMA((2,)),
            pltpu.SemaphoreType.DMA,
            pltpu.SemaphoreType.DMA((4,)),
            pltpu.SemaphoreType.DMA((4,)),
            pltpu.SemaphoreType.DMA((2, 8)),
            pltpu.SemaphoreType.DMA((2, 8)),
        ],
        compiler_params=pltpu.CompilerParams(
            collective_id=0, has_side_effects=True, vmem_limit_bytes=36 << 20
        ),
        cost_estimate=pl.CostEstimate(
            flops=2**32, bytes_accessed=12 << 20, transcendentals=0
        ),
        name="transform",
    )(*far)
    return pl.pallas_call(
        finish_kernel,
        in_specs=[pl.BlockSpec(memory_space=pltpu.VMEM)] * 3,
        out_specs=anywhere,
        out_shape=jax.ShapeDtypeStruct((2, 2, 8, 256, 2, 256), BF),
        scratch_shapes=[
            pltpu.VMEM((8, 256, 2, 256), BF),
            pltpu.SemaphoreType.DMA((3,)),
            pltpu.SemaphoreType.DMA((2,)),
        ],
        compiler_params=pltpu.CompilerParams(vmem_limit_bytes=26 << 20),
        cost_estimate=pl.CostEstimate(
            flops=2**30, bytes_accessed=8 << 20, transcendentals=0
        ),
        name="finish",
    )(ready, last, left)


def solution(mesh):
    return jax.shard_map(
        shards,
        mesh=mesh,
        in_specs=(P("tm", "lat", None), P(("tm", "lat"), None, None), P(), P()),
        out_specs=P(("tm", "lat"), None, None, None, None, None),
        check_vma=False,
    )
```

```python
import math

import jax
import jax.numpy as jnp
import numpy as np
from jax import lax
from jax.experimental import pallas as pl
from jax.experimental.pallas import tpu as pltpu
from jax.sharding import PartitionSpec as P

BF = jnp.bfloat16
F32 = jnp.float32


def longitude_table():
    group, op, slot = np.meshgrid(
        np.arange(4), np.arange(4), np.arange(32), indexing="ij"
    )
    order = (2 * (32 * group + slot) + op // 2).reshape(-1)
    part = (op % 2).reshape(-1)
    phase = np.arange(1024)[:, None] * order[None, :] % 1024
    angle = phase * (2.0 * math.pi / 1024)
    table = np.where(part[None, :] == 0, np.cos(angle), -np.sin(angle))
    return jnp.asarray((table / 32.0).astype(np.float32)).astype(BF)


def farthest_first(count, fields):
    def hops(i):
        return sum((0, 1, 2, 1)[i >> shift & 3] for shift in fields)

    return sorted(range(1, count), key=lambda i: (-hops(i), i))


UP = farthest_first(8, (1,))
ACROSS = farthest_first(16, (0, 2))


def swap_index_and_lanes(values, unit):
    values = list(values)
    lane = lax.broadcasted_iota(jnp.int32, values[0].shape, 1)
    step = len(values) // 2
    while step:
        low = (lane & (step * unit)) == 0
        for i in range(len(values)):
            if i & step == 0:
                a, b = values[i], values[i + step]
                values[i] = jnp.where(low, a, pltpu.roll(b, step * unit, 1))
                values[i + step] = jnp.where(
                    low, pltpu.roll(a, 128 - step * unit, 1), b
                )
        step //= 2
    return values


def transform_kernel(
    range_ref,
    offsets_ref,
    x_hbm,
    table_hbm,
    proj_hbm,
    out_ref,
    last_ref,
    left_ref,
    h_ref,
    left0_ref,
    x_ref,
    table_ref,
    proj_ref,
    flip_ref,
    up_ref,
    across_ref,
    via_up_ref,
    via_across_ref,
    r_ref,
    a_ref,
    part_ref,
    twice_ref,
    x_sem,
    table_sem,
    proj_sem,
    send_sem,
    recv_sem,
    pass_send_sem,
    pass_recv_sem,
):
    tm, lat = lax.axis_index("tm"), lax.axis_index("lat")
    me = 16 * tm + lat

    x_copies, table_copies = [], []
    for bh in range(2):
        for j in range(8):
            x_copies.append(
                pltpu.make_async_copy(
                    x_hbm.at[:, pl.ds(16 * bh, 16), pl.ds(128 * j, 128)],
                    x_ref.at[bh, j],
                    x_sem.at[bh, j],
                )
            )
    for j in range(2):
        table_copies.append(
            pltpu.make_async_copy(
                table_hbm.at[:, pl.ds(256 * j, 256)], table_ref.at[j], table_sem.at[j]
            )
        )
    proj_copy = pltpu.make_async_copy(proj_hbm, proj_ref, proj_sem)
    table_copies[0].start()
    for copy in x_copies[:8]:
        copy.start()
    table_copies[1].start()
    for copy in x_copies[8:]:
        copy.start()
    proj_copy.start()

    barrier = pltpu.get_barrier_semaphore()
    for i in range(1, 8):
        pl.semaphore_signal(barrier, inc=1, device_id=(tm ^ i, lat))
    for i in range(1, 16):
        pl.semaphore_signal(barrier, inc=1, device_id=(tm, lat ^ i))

    @pl.when((lat == 0) & (tm > 0))
    def _():
        pl.semaphore_signal(barrier, inc=1, device_id=(tm - 1, 15))

    @pl.when((lat == 15) & (tm < 7))
    def _():
        pl.semaphore_signal(barrier, inc=1, device_id=(tm + 1, 0))

    outside = ((lat == 0) & (tm > 0)) | ((lat == 15) & (tm < 7))

    def up(i, source, target, stage):
        return pltpu.make_async_remote_copy(
            src_ref=source,
            dst_ref=target,
            send_sem=send_sem.at[stage],
            recv_sem=recv_sem.at[stage],
            device_id=(tm ^ i, lat),
        )

    def across(i, source, target, stage):
        return pltpu.make_async_remote_copy(
            src_ref=source,
            dst_ref=target,
            send_sem=send_sem.at[stage],
            recv_sem=recv_sem.at[stage],
            device_id=(tm, lat ^ i),
        )

    for bh in range(2):
        for copy in x_copies[8 * bh : 8 * bh + 8]:
            copy.wait()
        for gp in range(2):
            if bh == 0:
                table_copies[gp].wait()
            x = jnp.concatenate(
                [x_ref[bh, j].reshape(512, 128) for j in range(8)], axis=1
            )
            z = jnp.dot(x, table_ref[gp], preferred_element_type=F32)
            z = z.astype(BF).reshape(32, 16, 256)
            for c in range(2):
                v = [z[t, :, 128 * c : 128 * c + 128] for t in range(32)]
                v = swap_index_and_lanes(v, 1)
                for slot in range(32):
                    to_tm, to_lat = 2 * (2 * gp + c) + slot // 16, slot % 16
                    if bh == 0:
                        up_ref[to_tm, to_lat] = v[slot]
                    else:
                        across_ref[to_lat, to_tm] = v[slot]
        if bh == 0:
            pl.semaphore_wait(barrier, 22 + outside.astype(jnp.int32))
            for i in UP:
                up(i, up_ref.at[tm ^ i], via_up_ref.at[tm], 0).start()

    for i in ACROSS:
        across(i, across_ref.at[lat ^ i], via_across_ref.at[lat], 1).start()
    via_up_ref[tm] = up_ref[tm]
    via_across_ref[lat] = across_ref[lat]

    proj_copy.wait()
    for o in range(2):
        bands = proj_ref[o].reshape(16, 2, 16, 256)
        for half in range(2):
            flip_ref[o, :, 256 * half : 256 * half + 256] = (
                bands[:, half].reshape(256, 256).T
            )

    some = pl.ds(0, 7)
    up_all = up(0, up_ref.at[some], via_up_ref.at[some], 0)
    up_all.wait_recv()
    for i in ACROSS:
        across(i, via_up_ref.at[:, lat ^ i], r_ref.at[:, lat, 0], 2).start()
    some = pl.ds(0, 15)
    across_all = across(0, across_ref.at[some], via_across_ref.at[some], 1)
    across_all.wait_recv()
    for i in UP:
        up(i, via_across_ref.at[:, tm ^ i], r_ref.at[tm, :, 1], 3).start()
    r_ref[:, lat, 0] = via_up_ref[:, lat]
    r_ref[tm, :, 1] = via_across_ref[:, tm]

    across_last = across(
        0, via_across_ref.at[pl.ds(0, 15)], r_ref.at[:, pl.ds(0, 15), 0], 2
    )
    up_last = up(0, via_up_ref.at[pl.ds(0, 7)], r_ref.at[pl.ds(0, 7), :, 1], 3)
    for half in range(2):
        if half == 0:
            across_last.wait_recv()
        else:
            up_last.wait_recv()
        for i in range(16):
            rows = slice(256 * half + 16 * i, 256 * half + 16 * i + 16)
            for q in range(2):
                v = [r_ref[4 * q + j, i, half] for j in range(4)]
                v = swap_index_and_lanes(v, 32)
                for op in range(4):
                    a_ref[op // 2, 2 * (op % 2) + q, rows, :] = v[op]
        if half == 0:
            for o in range(2):
                columns = jnp.concatenate([a_ref[o, j, :256] for j in range(4)], axis=1)
                part_ref[o] = jnp.dot(
                    flip_ref[o, :, :256], columns, preferred_element_type=F32
                )
    degree = lax.broadcasted_iota(jnp.int32, (256, 512), 0)
    before = jnp.maximum(me - 1, 0)

    def passed(o, c):
        rows = pl.ds(32 * c, 32)
        return pltpu.make_async_remote_copy(
            src_ref=h_ref.at[o, rows],
            dst_ref=h_ref.at[2 + o, rows],
            send_sem=pass_send_sem.at[o, c],
            recv_sem=pass_recv_sem.at[o, c],
            device_id=(before >> 4, before & 15),
        )

    for o in range(2):
        columns = jnp.concatenate([a_ref[o, j, 256:] for j in range(4)], axis=1)
        h = part_ref[o] + jnp.dot(
            flip_ref[o, :, 256:], columns, preferred_element_type=F32
        )
        low, high = range_ref[0, 2 * me + o], range_ref[1, 2 * me + o]
        keep = (degree >= low) & (degree < high)
        h_ref[o] = jnp.where(keep, h, 0.0).astype(BF)
        for c in range(8):

            @pl.when((me > 0) & (32 * (c + 1) > 2 * me + o))
            def _():
                passed(o, c).start()

    up_all.wait_send()
    across_all.wait_send()
    across_last.wait_send()
    up_last.wait_send()

    row = lax.broadcasted_iota(jnp.int32, (512, 256), 0)
    column = lax.broadcasted_iota(jnp.int32, (512, 256), 1)
    double = ((row >> 1) == column).astype(F32).astype(BF)
    for o in range(2):
        twice_ref[o] = jnp.dot(double, h_ref[o], preferred_element_type=F32)

    def build(o, k, target):
        cos, sin = phases(offsets_ref[k])
        cos = jnp.broadcast_to(cos[None], (64, 8, 256)).reshape(512, 256)
        sin = jnp.broadcast_to(sin[None], (64, 8, 256)).reshape(512, 256)
        real, imag = twice_ref[o, :, :256], twice_ref[o, :, 256:]
        target[k, :, :256] = (real * cos - imag * sin).astype(BF)
        target[k, :, 256:] = (real * sin + imag * cos).astype(BF)

    @pl.loop(0, 8)
    def _(k):
        build(0, k, left0_ref)

    def couple(place, left, partner, with_build=False):
        @pl.loop(0, 2)
        def _(half):
            for i in range(4):
                if with_build:
                    build(1, 4 * half + i, left_ref)
                product = lax.dot_general(
                    left[4 * half + i],
                    h_ref[partner],
                    (((1,), (1,)), ((), ())),
                    preferred_element_type=F32,
                )
                out_ref[place, 4 * half + i] = product.astype(BF).reshape(256, 2, 256)

    def receive(o):
        for c in range(8):
            sent = (me < 127) & (32 * (c + 1) > 2 * (me + 1) + o)

            @pl.when(sent)
            def _():
                passed(o, c).wait_recv()

            @pl.when(jnp.logical_not(sent))
            def _():
                h_ref[2 + o, 32 * c : 32 * c + 32] = jnp.zeros((32, 512), BF)

    couple(0, left0_ref, 1, with_build=True)
    receive(0)
    couple(1, left0_ref, 2)
    couple(2, left_ref, 2)
    receive(1)
    last_ref[...] = h_ref[3]
    for o in range(2):
        for c in range(8):

            @pl.when((me > 0) & (32 * (c + 1) > 2 * me + o))
            def _():
                passed(o, c).wait_send()


def phases(offset):
    row = lax.broadcasted_iota(jnp.int32, (8, 256), 0)
    t = lax.broadcasted_iota(jnp.int32, (8, 256), 1)
    turn = (offset * t + 64 * (row & 1)) & 255
    angle = turn.astype(F32) * (2.0 * math.pi / 256)
    return jnp.cos(angle) * (1.0 / 16), jnp.sin(angle) * (1.0 / 16)


def finish_kernel(out_ref, last_ref, left_ref, out_hbm, block_ref, early_sem, late_sem):
    early = [
        pltpu.make_async_copy(out_ref.at[i], out_hbm.at[o, s], early_sem.at[i])
        for i, (o, s) in enumerate(((0, 0), (0, 1), (1, 0)))
    ]
    for copy in early:
        copy.start()

    def late(half):
        some = pl.ds(4 * half, 4)
        return pltpu.make_async_copy(
            block_ref.at[some], out_hbm.at[1, 1, some], late_sem.at[half]
        )

    @pl.loop(0, 2)
    def _(half):
        for i in range(4):
            product = lax.dot_general(
                left_ref[4 * half + i],
                last_ref[...],
                (((1,), (1,)), ((), ())),
                preferred_element_type=F32,
            )
            block_ref[4 * half + i] = product.astype(BF).reshape(256, 2, 256)
        late(half).start()

    for copy in early:
        copy.wait()
    for half in range(2):
        late(half).wait()


def shards(frames, projection, degree_range, offsets):
    anywhere = pl.BlockSpec(memory_space=pltpu.HBM)
    far = [
        pltpu.with_memory_space_constraint(a, pltpu.HBM)
        for a in (degree_range.T, offsets, frames, longitude_table(), projection)
    ]
    ready, last, left = pl.pallas_call(
        transform_kernel,
        in_specs=[pl.BlockSpec(memory_space=pltpu.SMEM)] * 2 + [anywhere] * 3,
        out_specs=[pl.BlockSpec(memory_space=pltpu.VMEM)] * 3,
        out_shape=[
            jax.ShapeDtypeStruct((3, 8, 256, 2, 256), BF),
            jax.ShapeDtypeStruct((256, 512), BF),
            jax.ShapeDtypeStruct((8, 512, 512), BF),
        ],
        scratch_shapes=[
            pltpu.VMEM((4, 256, 512), BF),
            pltpu.VMEM((8, 512, 512), BF),
            pltpu.VMEM((2, 8, 32, 16, 128), BF),
            pltpu.VMEM((2, 1024, 256), BF),
            pltpu.VMEM((2, 512, 256), BF),
            pltpu.VMEM((2, 256, 512), BF),
            pltpu.VMEM((8, 16, 16, 128), BF),
            pltpu.VMEM((16, 8, 16, 128), BF),
            pltpu.VMEM((8, 16, 16, 128), BF),
            pltpu.VMEM((16, 8, 16, 128), BF),
            pltpu.VMEM((8, 16, 2, 16, 128), BF),
            pltpu.VMEM((2, 4, 512, 128), BF),
            pltpu.VMEM((2, 256, 512), F32),
            pltpu.VMEM((2, 512, 512), F32),
            pltpu.SemaphoreType.DMA((2, 8)),
            pltpu.SemaphoreType.DMA((2,)),
            pltpu.SemaphoreType.DMA,
            pltpu.SemaphoreType.DMA((4,)),
            pltpu.SemaphoreType.DMA((4,)),
            pltpu.SemaphoreType.DMA((2, 8)),
            pltpu.SemaphoreType.DMA((2, 8)),
        ],
        compiler_params=pltpu.CompilerParams(
            collective_id=0, has_side_effects=True, vmem_limit_bytes=36 << 20
        ),
        cost_estimate=pl.CostEstimate(
            flops=2**32, bytes_accessed=12 << 20, transcendentals=0
        ),
        name="transform",
    )(*far)
    return pl.pallas_call(
        finish_kernel,
        in_specs=[pl.BlockSpec(memory_space=pltpu.VMEM)] * 3,
        out_specs=anywhere,
        out_shape=jax.ShapeDtypeStruct((2, 2, 8, 256, 2, 256), BF),
        scratch_shapes=[
            pltpu.VMEM((8, 256, 2, 256), BF),
            pltpu.SemaphoreType.DMA((3,)),
            pltpu.SemaphoreType.DMA((2,)),
        ],
        compiler_params=pltpu.CompilerParams(vmem_limit_bytes=26 << 20),
        cost_estimate=pl.CostEstimate(
            flops=2**30, bytes_accessed=8 << 20, transcendentals=0
        ),
        name="finish",
    )(ready, last, left)


def solution(mesh):
    return jax.shard_map(
        shards,
        mesh=mesh,
        in_specs=(P("tm", "lat", None), P(("tm", "lat"), None, None), P(), P()),
        out_specs=P(("tm", "lat"), None, None, None, None, None),
        check_vma=False,
    )
```
